256 devices in a mesh: ens: 8 (over z_hi, y), gy: 4 (over z_lo), gx: 8 (over x, core).
Axes of the slice: x: 4, y: 4, z: 8 (z_hi: 2, z_lo: 4; z = z_hi * 4 + z_lo), core: 2. Of those that a mesh axis runs over, the one named last changes fastest.
Arguments:
- velocity: float32 [8, 2, 1024, 2048], P('ens', None, 'gy', 'gx'), may hold values from -3 to 3
- stress: float32 [8, 3, 1024, 2048], P('ens', None, 'gy', 'gx'), may hold values from -3 to 3
- thickness: float32 [8, 1024, 2048], P('ens', 'gy', 'gx'), may hold values from 2 to 3
- concentration: float32 [8, 1024, 2048], P('ens', 'gy', 'gx'), may hold values from 0.97 to 1
- node_mass: float32 [8, 1024, 2048], P('ens', 'gy', 'gx'), may hold values from 1 to 1.5
- wind_stress: float32 [8, 2, 1024, 2048], P('ens', None, 'gy', 'gx'), may hold values from -3 to 3
- ocean_current: float32 [8, 2, 1024, 2048], P('ens', None, 'gy', 'gx'), may hold values from -2 to 2
- ocean_mask: int32 [1024, 2048], P('gy', 'gx'), may hold values 0 or 1
- ice_blocks: int32 [8, 32, 64], P('ens', 'gy', 'gx'), may hold values 0 or 1
Outputs:
- velocity_out: float32 [8, 2, 1024, 2048], P('ens', None, 'gy', 'gx')
- stress_out: float32 [8, 3, 1024, 2048], P('ens', None, 'gy', 'gx')
- ensemble_mean: float32 [3, 1024, 2048], P(None, ('gy', 'ens'), 'gx')
- ensemble_variance: float32 [3, 1024, 2048], P(None, ('gy', 'ens'), 'gx')
The draws below stay inside these ranges and needn't reach their ends.
All inputs are finite; a program needn't handle non-finite values. No bound on the sum of `ocean_mask` or of `ice_blocks` on one device may be relied on, other than what follows from the above.
Results may differ from the reference program's by a relative error of at most 0.00002.
Values sent between devices are 32-bit elements; how exact they have to be, the bound alone decides.
A program may use at most 64 MiB of HBM per device.

```python
import math
import jax
import jax.numpy as jnp
from jax import lax

SUBCYCLES = 16
BLOCK = 32
MEMBERS = 8
NX = 2048
NY = 1024


def place_ends(entries, stream_key, low, high):
    extent = entries.shape
    place = [jax.random.randint(jax.random.fold_in(stream_key, axis), (), 0, extent[axis]) for axis in range(len(extent))]
    entries = entries.at[tuple(place)].set(low)
    longest = extent.index(max(extent))
    place[longest] = (place[longest] + 1) % extent[longest]
    return entries.at[tuple(place)].set(high)


def block_levels(key, dims, shards, smallest, largest):
    factor_of, own = 1.0, jax.random.fold_in(key, 6)
    for axis_at, shards_of in shards:
        draws = jnp.exp(jax.random.uniform(jax.random.fold_in(own, axis_at), (shards_of,), jnp.float32, smallest / len(shards), largest / len(shards)))
        factor_of = factor_of * jnp.repeat(draws, dims[axis_at] // shards_of).reshape([-1 if axis == axis_at else 1 for axis in range(len(dims))])
    return factor_of


def normal_values(rng, shape, scale, most, shards=(), kind=jnp.bfloat16):
    entries = jax.random.normal(rng, shape, jnp.float32) * scale
    if len(shards) > 0:
        entries = block_levels(rng, shape, shards, -0.22, 0.18) * entries
    return jnp.clip(entries, min=-most, max=most).astype(kind)


def setup_inputs(seed: int = 0) -> dict:
    key_list = jax.random.split(jax.random.key(seed), 10)
    return {
        "velocity": normal_values(key_list[0], (MEMBERS, 2, NY, NX), 0.5, 3.0, ((0, 8), (2, 4), (3, 8)), jnp.float32),
        "stress": normal_values(key_list[1], (MEMBERS, 3, NY, NX), 0.5, 3.0, ((0, 8), (2, 4), (3, 8)), jnp.float32),
        "thickness": jnp.clip(jnp.exp(math.log(3.0) - 0.4054651 * jax.random.uniform(key_list[2], (MEMBERS, NY, NX), jnp.float32) ** block_levels(key_list[2], (MEMBERS, NY, NX), ((0, 8), (1, 4), (2, 8)), -0.2, 0.2)), 2.0, 3.0),
        "concentration": jnp.clip(0.97 + 0.029999971 * jax.random.uniform(key_list[3], (MEMBERS, NY, NX), jnp.float32) ** block_levels(key_list[3], (MEMBERS, NY, NX), ((0, 8), (1, 4), (2, 8)), -0.2, 0.2), 0.97, 1.0),
        "node_mass": jnp.clip(jnp.exp(math.log(1.5) - 0.4054651 * jax.random.uniform(key_list[4], (MEMBERS, NY, NX), jnp.float32) ** block_levels(key_list[4], (MEMBERS, NY, NX), ((0, 8), (1, 4), (2, 8)), -0.2, 0.2)), 1.0, 1.5),
        "wind_stress": normal_values(key_list[5], (MEMBERS, 2, NY, NX), 0.5, 3.0, ((0, 8), (2, 4), (3, 8)), jnp.float32),
        "ocean_current": normal_values(key_list[6], (MEMBERS, 2, NY, NX), 0.3, 2.0, ((0, 8), (2, 4), (3, 8)), jnp.float32),
        "ocean_mask": place_ends((jax.random.randint(key_list[7], (NY, NX), 0, 5) < 4).astype(jnp.int32), jax.random.fold_in(key_list[7], 1), 0, 1),
        "ice_blocks": place_ends((jax.random.randint(key_list[8], (MEMBERS, NY // BLOCK, NX // BLOCK), 0, 4) < 3).astype(jnp.int32), jax.random.fold_in(key_list[8], 1), 0, 1),
    }


TIME_STEP = 0.5
RELAX_RATE = 0.25
ECCENTRICITY_SQUARED = 4.0
DELTA_FLOOR = 0.5
DRAG_WATER = 1.0
CORIOLIS_TOP = 1.0
STRENGTH_DECAY = 20.0
ADVECT_STEP = 1.0

def upper_extend(source):
    wrapped = jnp.concatenate([source, source[..., :1]], axis=-1)
    zeros_row = jnp.zeros_like(wrapped[..., :1, :])
    return jnp.concatenate([wrapped, zeros_row], axis=-2)

def lower_extend(source):
    wrapped = jnp.concatenate([source[..., -1:], source], axis=-1)
    zeros_row = jnp.zeros_like(wrapped[..., :1, :])
    return jnp.concatenate([zeros_row, wrapped], axis=-2)

def along_x(nodal_field):
    return 0.5 * (nodal_field[..., :-1, 1:] + nodal_field[..., 1:, 1:] - (nodal_field[..., :-1, :-1] + nodal_field[..., 1:, :-1]))

def along_y(nodal_field):
    return 0.5 * (nodal_field[..., 1:, :-1] + nodal_field[..., 1:, 1:] - (nodal_field[..., :-1, :-1] + nodal_field[..., :-1, 1:]))

def stress_update(stresses, extended_vel, strength):
    divergence = along_x(extended_vel[:, 0]) + along_y(extended_vel[:, 1])
    tension = along_x(extended_vel[:, 0]) - along_y(extended_vel[:, 1])
    shearing = along_y(extended_vel[:, 0]) + along_x(extended_vel[:, 1])
    deform = jnp.sqrt(divergence * divergence + (tension * tension + shearing * shearing) / ECCENTRICITY_SQUARED)
    bounded = jnp.maximum(deform, DELTA_FLOOR)
    weight = RELAX_RATE * 0.5 * strength / bounded
    stress_one = (stresses[:, 0] + weight * (divergence - deform)) / (1.0 + RELAX_RATE)
    stress_two = (stresses[:, 1] + weight * tension / ECCENTRICITY_SQUARED) / (1.0 + RELAX_RATE)
    stress_three = (stresses[:, 2] + weight * shearing / (2.0 * ECCENTRICITY_SQUARED)) / (1.0 + RELAX_RATE)
    return jnp.stack([stress_one, stress_two, stress_three], axis=1)

def momentum_update(moving, extended_stress, node_mass, wind_stress, ocean_current, coriolis, active):
    normal_east = 0.5 * (extended_stress[:, 0] + extended_stress[:, 1])
    normal_north = 0.5 * (extended_stress[:, 0] - extended_stress[:, 1])
    shear_part = extended_stress[:, 2]
    force_east = along_x(normal_east) + along_y(shear_part)
    force_north = along_x(shear_part) + along_y(normal_north)
    east_vel = moving[:, 0]
    north_vel = moving[:, 1]
    current_east = ocean_current[:, 0]
    current_north = ocean_current[:, 1]
    drag_rate = DRAG_WATER * jnp.sqrt((current_east - east_vel) * (current_east - east_vel) + (current_north - north_vel) * (current_north - north_vel))
    inertia = node_mass / TIME_STEP
    diagonal_term = inertia + drag_rate
    turning = coriolis * node_mass
    rhs_east = inertia * east_vel + force_east + wind_stress[:, 0] + drag_rate * current_east
    rhs_north = inertia * north_vel + force_north + wind_stress[:, 1] + drag_rate * current_north
    determinant = diagonal_term * diagonal_term + turning * turning
    new_east = active * (diagonal_term * rhs_east + turning * rhs_north) / determinant
    new_north = active * (diagonal_term * rhs_north - turning * rhs_east) / determinant
    return jnp.stack([new_east, new_north], axis=1)

def reference(velocity, stress, thickness, concentration, node_mass, wind_stress, ocean_current, ocean_mask, ice_blocks):
    present = jnp.repeat(jnp.repeat(ice_blocks, BLOCK, axis=1), BLOCK, axis=2).astype(jnp.float32)
    active = ocean_mask.astype(jnp.float32)[None] * present
    strength = thickness * jnp.exp(-STRENGTH_DECAY * (1.0 - concentration))
    row_index = jnp.arange(NY, dtype=jnp.int32).astype(jnp.float32)
    coriolis = (CORIOLIS_TOP * (row_index + 0.5) / NY)[:, None]
    initial = velocity * active[:, None]

    def subcycle(counter, carried):
        moving, stresses = carried
        stresses = stress_update(stresses, upper_extend(moving), strength)
        moving = momentum_update(moving, lower_extend(stresses), node_mass, wind_stress, ocean_current, coriolis, active)
        return (moving, stresses)
    final_vel, final_stress = lax.fori_loop(0, SUBCYCLES, subcycle, (initial, stress))
    extended = upper_extend(final_vel)
    divergence = along_x(extended[:, 0]) + along_y(extended[:, 1])
    drifted = jnp.clip(concentration - ADVECT_STEP * concentration * divergence, 0.0, 1.0)
    fields = jnp.stack([drifted, final_vel[:, 0], final_vel[:, 1]], axis=1)
    average = lax.optimization_barrier(jnp.sum(fields, axis=0)) / MEMBERS
    deviation = fields - average[None]
    spread = lax.optimization_barrier(jnp.sum(deviation * deviation, axis=0)) / MEMBERS
    return (final_vel, final_stress, average, spread)
```

```python
import functools
import math

import jax
import jax.numpy as jnp
from jax import lax
from jax.experimental import pallas as pl
from jax.experimental.pallas import tpu as pltpu
from jax.sharding import PartitionSpec as P

SUBCYCLES = 16
RELAX = 0.25
DECAY = 20.0
FLOOR = 0.5
ROOT2 = math.sqrt(2.0)
BETA = 1.0 / (4.0 * ROOT2)
KEEP = 1.0 / (1.0 + RELAX)
GAIN = BETA * 0.5 * RELAX * KEEP
TINY = 1.1754944e-38

LANES = 128
ROWS = 256
BASE = 24
HALO = 16
ALLOC = 312
FIRST, LAST = 1, 37
W, Z, PP, MM, TT, SM, MA, WW, WZ, CW, CZ, B2, BB = range(13)
SENT = 12
PITCH = 20
LAG = 8
MESH_IDS = pl.DeviceIdType.MESH


def lane_ids():
    return lax.broadcasted_iota(jnp.int32, (8, LANES), 1)


def tile(r):
    return pl.ds(r, 8)


def sweep(F, RL, tiles, first, last, lag):
    lane = lane_ids()
    low, high = lane == 0, lane == LANES - 1

    def ld(f, q, r):
        return F[f, q, tile(r), :]

    def rl(f, q, r):
        return RL[f, q, tile(r), :]

    def turn(dst, src, t, shift, edge):
        values = [pltpu.roll(ld(src, q, 8 * t), shift, 1) for q in tiles]
        if len(tiles) == 2:
            values = [jnp.where(edge, values[1 - n], values[n]) for n in range(2)]
        for q, value in zip(tiles, values):
            RL[dst, q, tile(8 * t), :] = value

    def stress(t):
        r = 8 * t
        for q in tiles:
            w, wd = ld(W, q, r), ld(W, q, r + 1)
            z, zd = ld(Z, q, r), ld(Z, q, r + 1)
            w1, w1d = rl(0, q, r), rl(0, q, r + 1)
            z1, z1d = rl(1, q, r), rl(1, q, r + 1)
            a, b, c, d = w1d - w, z1 - zd, z1d - z, w1 - wd
            div, shear, tension = a + b, a - b, c + d
            s4, t4 = shear * 0.25, tension * 0.25
            square = div * div + (shear * s4 + tension * t4)
            inverse = lax.rsqrt(jnp.maximum(square, TINY))
            e = div - square * inverse
            g = ld(SM, q, r) * jnp.minimum(inverse, 1.0 / FLOOR)
            F[PP, q, tile(r), :] = ld(PP, q, r) * KEEP + g * (e + s4)
            F[MM, q, tile(r), :] = ld(MM, q, r) * KEEP + g * (e - s4)
            F[TT, q, tile(r), :] = ld(TT, q, r) * KEEP + g * t4
        for dst, src in ((2, PP), (3, MM), (4, TT)):
            turn(dst, src, t, 1, low)

    def momentum(t):
        r = 8 * t
        for q in tiles:
            fw = (ld(PP, q, r) - rl(2, q, r - 1)) + (ld(TT, q, r - 1) - rl(4, q, r))
            fz = (ld(TT, q, r) - rl(4, q, r - 1)) + (ld(MM, q, r - 1) - rl(3, q, r))
            w, z = ld(W, q, r), ld(Z, q, r)
            cw, cz = ld(CW, q, r), ld(CZ, q, r)
            dw, dz = cw - w, cz - z
            dq = dw * dw + dz * dz
            drag = dq * lax.rsqrt(jnp.maximum(dq, TINY))
            mass, b = ld(MA, q, r), ld(BB, q, r)
            a = mass + drag
            rw = (mass * w + drag * cw) + (fw + ld(WW, q, r))
            rz = (mass * z + drag * cz) + (fz + ld(WZ, q, r))
            root = lax.rsqrt(a * a + ld(B2, q, r))
            quotient = root * root
            a, b = a * quotient, b * quotient
            F[W, q, tile(r), :] = a * rw - b * rz
            F[Z, q, tile(r), :] = a * rz + b * rw
        for dst, src in ((0, W), (1, Z)):
            turn(dst, src, t, LANES - 1, high)

    for k in range(last - first + lag):
        if first + k < last:
            stress(first + k)
        if k >= lag:
            momentum(first + k - lag)


def kernel(
    vel_h, st_h, thick_h, conc_h, mass_h, wind_h, cur_h, mask_h, ice_s,
    vel_o, st_o, conc_o,
    F, RL, IN, MK, SP, RP, OUT,
    load_sem, send_sem, recv_sem, out_sem,
):
    gx, gy = lax.axis_index("gx"), lax.axis_index("gy")
    nx, ny = lax.axis_size("gx"), lax.axis_size("gy")
    left, right = lax.rem(gx + nx - 1, nx), lax.rem(gx + 1, nx)
    has_down, has_up = gy > 0, gy < ny - 1
    lane = lane_ids()
    halves = (pl.ds(0, LANES), pl.ds(LANES, LANES))
    whole = pl.ds(0, ROWS)

    sources = [vel_h.at[0, 0], vel_h.at[0, 1], st_h.at[0, 0], st_h.at[0, 1], st_h.at[0, 2],
               thick_h.at[0], conc_h.at[0], mass_h.at[0], wind_h.at[0, 0], wind_h.at[0, 1],
               cur_h.at[0, 0], cur_h.at[0, 1]]
    loads = []
    for n, source in enumerate(sources):
        for q in range(2):
            loads.append(pltpu.make_async_copy(
                source.at[whole, halves[q]], IN.at[n, q], load_sem.at[2 * n + q]))
    for q in range(2):
        loads.append(pltpu.make_async_copy(
            mask_h.at[whole, halves[q]], MK.at[q], load_sem.at[24 + q]))
    for copy in loads:
        copy.start()

    barrier = pltpu.get_barrier_semaphore()
    for neighbour in (left, right):
        pl.semaphore_signal(barrier, inc=1, device_id={"gx": neighbour}, device_id_type=MESH_IDS)

    @pl.when(has_down)
    def _():
        pl.semaphore_signal(barrier, inc=1, device_id={"gy": gy - 1}, device_id_type=MESH_IDS)

    @pl.when(has_up)
    def _():
        pl.semaphore_signal(barrier, inc=1, device_id={"gy": gy + 1}, device_id_type=MESH_IDS)

    zero = jnp.zeros((8, LANES), jnp.float32)
    for f in (PP, MM, TT):
        for q in range(3):
            F[f, q, tile(0), :] = zero
    for f in (2, 3, 4):
        for q in range(3):
            RL[f, q, tile(0), :] = zero

    for copy in loads:
        copy.wait()

    def slot_mask(start, width):
        return lax.rem(lane - start + 2 * LANES, LANES) < width

    def derive(block, carry):
        present = []
        for q in range(2):
            c = [ice_s[0, block, 4 * q + n] for n in range(4)]
            present.append(jnp.where(
                lane < 64, jnp.where(lane < 32, c[0], c[1]), jnp.where(lane < 96, c[2], c[3])))
        for n in range(4):
            r = pl.multiple_of(block * 32 + 8 * n, 8)
            fields = []
            for q in range(2):
                u, v, s0, s1, s2, thick, conc, mass, we, wn, ce, cn = (
                    IN[f, q, tile(r), :] for f in range(12))
                active = (MK[q, tile(r), :] * present[q]).astype(jnp.float32)
                u, v = u * active, v * active
                strength = thick * jnp.exp(-DECAY * (1.0 - conc))
                s0, s2 = s0 * BETA, s2 * (2.0 * BETA)
                scale = 0.5 / ROOT2
                fields.append((
                    0.5 * (u + v), 0.5 * (u - v), s0 + s2, s0 - s2, s1 * BETA, strength * GAIN,
                    mass * ROOT2, scale * (we + wn), scale * (we - wn),
                    0.5 * (ce + cn), 0.5 * (ce - cn), active))
                for f in range(SENT):
                    F[f, q, tile(r + BASE), :] = fields[q][f]
            for part in range(2):
                to_left = to_right = None
                for s in range(6):
                    f = 6 * part + s
                    low = pltpu.roll(fields[0][f], PITCH * s, 1) if s else fields[0][f]
                    high = pltpu.roll(fields[1][f], (PITCH * s + 33) % LANES, 1)
                    if s == 0:
                        to_left, to_right = low, high
                    else:
                        to_left = jnp.where(slot_mask(PITCH * s, 17), low, to_left)
                        to_right = jnp.where(slot_mask(PITCH * s + 17, 16), high, to_right)
                SP[0, part, tile(r), :] = to_left
                SP[1, part, tile(r), :] = to_right
        return carry

    lax.fori_loop(0, ROWS // 32, derive, 0)

    pl.semaphore_wait(barrier, 2 + has_down.astype(jnp.int32) + has_up.astype(jnp.int32))

    to_left = pltpu.make_async_remote_copy(
        SP.at[0], RP.at[0], send_sem.at[0], recv_sem.at[0],
        device_id={"gx": left}, device_id_type=MESH_IDS)
    to_right = pltpu.make_async_remote_copy(
        SP.at[1], RP.at[1], send_sem.at[1], recv_sem.at[1],
        device_id={"gx": right}, device_id_type=MESH_IDS)
    to_left.start()
    to_right.start()

    def row_copies(q, count, n):
        planes = pl.ds(q, count)

        def part(f0, nf, src, dst, rows, slot, row):
            return pltpu.make_async_remote_copy(
                F.at[pl.ds(f0, nf), planes, pl.ds(src, rows)],
                F.at[pl.ds(f0, nf), planes, pl.ds(dst, rows)],
                send_sem.at[slot], recv_sem.at[slot],
                device_id={"gy": row}, device_id_type=MESH_IDS)

        down = [part(0, SENT, BASE, BASE + ROWS, HALO, n, gy - 1),
                part(0, 2, BASE + HALO, BASE + ROWS + HALO, 8, n + 1, gy - 1)]
        up = [part(0, SENT, BASE + ROWS - HALO, BASE - HALO, HALO, n + 2, gy + 1)]
        return down, up

    main_down, main_up = row_copies(0, 2, 2)
    strip_down, strip_up = row_copies(2, 1, 5)

    def start_rows(down, up):
        @pl.when(has_down)
        def _():
            for copy in down:
                copy.start()

        @pl.when(has_up)
        def _():
            for copy in up:
                copy.start()

    def wait_rows(down, up):
        @pl.when(has_down)
        def _():
            for copy in down:
                copy.wait_send()
            for copy in up:
                copy.wait_recv()

        @pl.when(has_up)
        def _():
            for copy in up:
                copy.wait_send()
            for copy in down:
                copy.wait_recv()

    start_rows(main_down, main_up)
    to_left.wait_recv()
    to_right.wait_recv()

    def build(block, carry):
        for n in range(2):
            r = pl.multiple_of(block * 16 + 8 * n, 8)
            for part in range(2):
                from_right, from_left = RP[0, part, tile(r), :], RP[1, part, tile(r), :]
                for s in range(6):
                    f = 6 * part + s
                    both = jnp.where(slot_mask(PITCH * s + 17, 16), from_left, from_right)
                    both = pltpu.roll(both, (95 - PITCH * s) % LANES, 1)
                    high = pltpu.roll(F[f, 1, tile(r + BASE), :], 95, 1)
                    F[f, 2, tile(r + BASE), :] = jnp.where(
                        lane < 48, F[f, 0, tile(r + BASE), :], jnp.where(lane < 95, high, both))
        return carry

    lax.fori_loop(0, ROWS // 16, build, 0)
    start_rows(strip_down, strip_up)

    def outside(start, count):
        for f in range(SENT):
            value = jnp.ones((8, LANES), jnp.float32) if f == MA else zero
            for q in range(3):
                for n in range(count):
                    F[f, q, tile(start + 8 * n), :] = value

    @pl.when(jnp.logical_not(has_down))
    def _():
        outside(BASE - HALO, 2)

    @pl.when(jnp.logical_not(has_up))
    def _():
        outside(BASE + ROWS, 3)

    to_left.wait_send()
    to_right.wait_send()
    wait_rows(main_down, main_up)
    wait_rows(strip_down, strip_up)

    sub = lax.broadcasted_iota(jnp.int32, (8, LANES), 0)
    grid_rows = ny * ROWS

    def prepare(t, carry):
        r = pl.multiple_of(8 * t, 8)
        row = (sub + (gy * ROWS - BASE + r)).astype(jnp.float32) + 0.5
        half = row * (0.5 / grid_rows)
        for q in range(3):
            b = half * F[MA, q, tile(r), :]
            F[BB, q, tile(r), :] = b
            F[B2, q, tile(r), :] = jnp.where(F[B2, q, tile(r), :] > 0.5, b * b, jnp.inf)
        return carry

    lax.fori_loop(FIRST, LAST, prepare, 0)

    def turn_first(t, carry):
        r = pl.multiple_of(8 * t, 8)
        for dst, f in ((0, W), (1, Z)):
            v = [pltpu.roll(F[f, q, tile(r), :], LANES - 1, 1) for q in range(3)]
            RL[dst, 0, tile(r), :] = jnp.where(lane == LANES - 1, v[1], v[0])
            RL[dst, 1, tile(r), :] = jnp.where(lane == LANES - 1, v[0], v[1])
            RL[dst, 2, tile(r), :] = v[2]
        return carry

    lax.fori_loop(FIRST, LAST + 1, turn_first, 0)

    def main_cycle(n, carry):
        sweep(F, RL, (0, 1), FIRST, LAST, LAG)
        return carry

    def strip_cycle(n, carry):
        sweep(F, RL, (2,), FIRST, LAST, LAG)
        return carry

    lax.fori_loop(0, SUBCYCLES, main_cycle, 0)
    lax.fori_loop(0, SUBCYCLES, strip_cycle, 0)

    def finish(block, carry):
        for n in range(2):
            o = pl.multiple_of(block * 16 + 8 * n, 8)
            r = o + BASE

            def merged(values):
                low = jnp.where(lane < 16, values[2], values[0])
                high = jnp.where(lane >= 108, pltpu.roll(values[2], 33, 1), values[1])
                return low, high

            div = []
            for q in range(3):
                a = RL[0, q, tile(r + 1), :] - F[W, q, tile(r), :]
                b = RL[1, q, tile(r), :] - F[Z, q, tile(r + 1), :]
                div.append(a + b)
            div = merged(div)
            w, z, p, m, t = (
                merged([F[f, q, tile(r), :] for q in range(3)]) for f in (W, Z, PP, MM, TT))
            for q in range(2):
                conc = IN[6, q, tile(o), :]
                OUT[0, q, tile(o), :] = w[q] + z[q]
                OUT[1, q, tile(o), :] = w[q] - z[q]
                OUT[2, q, tile(o), :] = (p[q] + m[q]) * (0.5 / BETA)
                OUT[3, q, tile(o), :] = t[q] * (1.0 / BETA)
                OUT[4, q, tile(o), :] = (p[q] - m[q]) * (0.25 / BETA)
                OUT[5, q, tile(o), :] = jnp.clip(conc - conc * div[q], 0.0, 1.0)
        return carry

    lax.fori_loop(0, ROWS // 16, finish, 0)
    targets = [vel_o.at[0, 0], vel_o.at[0, 1], st_o.at[0, 0], st_o.at[0, 1], st_o.at[0, 2],
               conc_o.at[0]]
    stores = []
    for n, target in enumerate(targets):
        for q in range(2):
            stores.append(pltpu.make_async_copy(
                OUT.at[n, q], target.at[whole, halves[q]], out_sem.at[2 * n + q]))
    for copy in stores:
        copy.start()
    for copy in stores:
        copy.wait()


def body(velocity, stress, thickness, concentration, node_mass, wind_stress, ocean_current,
         ocean_mask, ice_blocks):
    f32 = jnp.float32
    anywhere = pl.BlockSpec(memory_space=pl.ANY)
    final_vel, final_stress, drifted = pl.pallas_call(
        kernel,
        out_shape=(
            jax.ShapeDtypeStruct(velocity.shape, f32),
            jax.ShapeDtypeStruct(stress.shape, f32),
            jax.ShapeDtypeStruct(concentration.shape, f32),
        ),
        in_specs=[anywhere] * 8 + [pl.BlockSpec(memory_space=pltpu.SMEM)],
        out_specs=(anywhere,) * 3,
        scratch_shapes=[
            pltpu.VMEM((13, 3, ALLOC, LANES), f32),
            pltpu.VMEM((5, 3, ALLOC, LANES), f32),
            pltpu.VMEM((12, 2, ROWS, LANES), f32),
            pltpu.VMEM((2, ROWS, LANES), jnp.int32),
            pltpu.VMEM((2, 2, ROWS, LANES), f32),
            pltpu.VMEM((2, 2, ROWS, LANES), f32),
            pltpu.VMEM((6, 2, ROWS, LANES), f32),
            pltpu.SemaphoreType.DMA((26,)),
            pltpu.SemaphoreType.DMA((8,)),
            pltpu.SemaphoreType.DMA((8,)),
            pltpu.SemaphoreType.DMA((12,)),
        ],
        compiler_params=pltpu.CompilerParams(
            collective_id=0, has_side_effects=True, vmem_limit_bytes=67043328),
        name="ice",
    )(velocity, stress, thickness, concentration, node_mass, wind_stress, ocean_current,
      ocean_mask, ice_blocks)
    fields = jnp.stack([drifted, final_vel[:, 0], final_vel[:, 1]], axis=1)
    members = lax.axis_size("ens")
    gathered = lax.all_to_all(fields, "ens", split_axis=2, concat_axis=0, tiled=True)
    mean = jnp.sum(gathered, axis=0) / members
    deviation = gathered - mean[None]
    spread = jnp.sum(deviation * deviation, axis=0) / members
    return final_vel, final_stress, mean, spread


def solution(mesh):
    member, field = P("ens", None, "gy", "gx"), P("ens", "gy", "gx")
    placed = (member, member, field, field, field, member, member, P("gy", "gx"), field)
    block = P(None, ("gy", "ens"), "gx")
    return jax.shard_map(
        body, mesh=mesh, in_specs=placed, out_specs=(member, member, block, block),
        check_vma=False)
```

```python
import functools
import math

import jax
import jax.numpy as jnp
from jax import lax
from jax.experimental import pallas as pl
from jax.experimental.pallas import tpu as pltpu
from jax.sharding import PartitionSpec as P

SUBCYCLES = 16
RELAX = 0.25
DECAY = 20.0
FLOOR = 0.5
ROOT2 = math.sqrt(2.0)
BETA = 1.0 / (4.0 * ROOT2)
KEEP = 1.0 / (1.0 + RELAX)
GAIN = BETA * 0.5 * RELAX * KEEP
TINY = 1.1754944e-38

LANES = 128
ROWS = 256
BASE = 24
HALO = 16
ALLOC = 312
FIRST, LAST = 1, 37
W, Z, PP, MM, TT, SM, MA, WW, WZ, CW, CZ, B2, BB = range(13)
SENT = 12
PITCH = 20
LAG = 8
EARLY = 8
CHUNK = 64
CTILES = CHUNK // 8 + 2
CLAG = 3
OWN = 32
MESH_IDS = pl.DeviceIdType.MESH


def lane_ids():
    return lax.broadcasted_iota(jnp.int32, (8, LANES), 1)


def tile(r):
    return pl.ds(r, 8)


def sweep(state, rolled, const, tiles, first, last, lag):
    lane = lane_ids()
    low, high = lane == 0, lane == LANES - 1
    (S, so), (RL, ro), (C, co) = state, rolled, const

    def ld(f, q, r):
        return S[f, q, tile(r + so), :]

    def rl(f, q, r):
        return RL[f, q, tile(r + ro), :]

    def const_of(f, q, r):
        return C[f, q, tile(r + co), :]

    def turn(dst, src, t, shift, edge):
        values = [pltpu.roll(ld(src, q, 8 * t), shift, 1) for q in tiles]
        if len(tiles) > 1:
            values[:2] = [jnp.where(edge, values[1 - n], values[n]) for n in range(2)]
        for q, value in zip(tiles, values):
            RL[dst, q, tile(8 * t + ro), :] = value

    def stress(t):
        r = 8 * t
        for q in tiles:
            w, wd = ld(W, q, r), ld(W, q, r + 1)
            z, zd = ld(Z, q, r), ld(Z, q, r + 1)
            w1, w1d = rl(0, q, r), rl(0, q, r + 1)
            z1, z1d = rl(1, q, r), rl(1, q, r + 1)
            a, b, c, d = w1d - w, z1 - zd, z1d - z, w1 - wd
            div, shear, tension = a + b, a - b, c + d
            s4, t4 = shear * 0.25, tension * 0.25
            square = div * div + (shear * s4 + tension * t4)
            inverse = lax.rsqrt(jnp.maximum(square, TINY))
            e = div - square * inverse
            g = const_of(SM, q, r) * jnp.minimum(inverse, 1.0 / FLOOR)
            S[PP, q, tile(r + so), :] = ld(PP, q, r) * KEEP + g * (e + s4)
            S[MM, q, tile(r + so), :] = ld(MM, q, r) * KEEP + g * (e - s4)
            S[TT, q, tile(r + so), :] = ld(TT, q, r) * KEEP + g * t4
        for dst, src in ((2, PP), (3, MM), (4, TT)):
            turn(dst, src, t, 1, low)

    def momentum(t):
        r = 8 * t
        for q in tiles:
            fw = (ld(PP, q, r) - rl(2, q, r - 1)) + (ld(TT, q, r - 1) - rl(4, q, r))
            fz = (ld(TT, q, r) - rl(4, q, r - 1)) + (ld(MM, q, r - 1) - rl(3, q, r))
            w, z = ld(W, q, r), ld(Z, q, r)
            cw, cz = const_of(CW, q, r), const_of(CZ, q, r)
            dw, dz = cw - w, cz - z
            dq = dw * dw + dz * dz
            drag = dq * lax.rsqrt(jnp.maximum(dq, TINY))
            mass, b = const_of(MA, q, r), const_of(BB, q, r)
            a = mass + drag
            rw = (mass * w + drag * cw) + (fw + const_of(WW, q, r))
            rz = (mass * z + drag * cz) + (fz + const_of(WZ, q, r))
            root = lax.rsqrt(a * a + const_of(B2, q, r))
            quotient = root * root
            a, b = a * quotient, b * quotient
            S[W, q, tile(r + so), :] = a * rw - b * rz
            S[Z, q, tile(r + so), :] = a * rz + b * rw
        for dst, src in ((0, W), (1, Z)):
            turn(dst, src, t, LANES - 1, high)

    for k in range(last - first + lag):
        if first + k < last:
            stress(first + k)
        if k >= lag:
            momentum(first + k - lag)


def kernel(
    vel_h, st_h, thick_h, conc_h, mass_h, wind_h, cur_h, mask_h, ice_s,
    vel_o, st_o, mean_o, var_o,
    F, RL, IN, MK, SP, RP, OUT, G, FB, YR, PART, ZR, STAT,
    load_sem, send_sem, recv_sem, out_sem, ysend_sem, yrecv_sem, zsend_sem, zrecv_sem,
):
    gx, gy = lax.axis_index("gx"), lax.axis_index("gy")
    nx, ny = lax.axis_size("gx"), lax.axis_size("gy")
    left, right = lax.rem(gx + nx - 1, nx), lax.rem(gx + 1, nx)
    has_down, has_up = gy > 0, gy < ny - 1
    lane = lane_ids()
    halves = (pl.ds(0, LANES), pl.ds(LANES, LANES))
    whole = pl.ds(0, ROWS)

    sources = [vel_h.at[0, 0], vel_h.at[0, 1], st_h.at[0, 0], st_h.at[0, 1], st_h.at[0, 2],
               thick_h.at[0], conc_h.at[0], mass_h.at[0], wind_h.at[0, 0], wind_h.at[0, 1],
               cur_h.at[0, 0], cur_h.at[0, 1]]
    loads = []
    for n, source in enumerate(sources):
        for q in range(2):
            loads.append(pltpu.make_async_copy(
                source.at[whole, halves[q]], IN.at[n, q], load_sem.at[2 * n + q]))
    for q in range(2):
        loads.append(pltpu.make_async_copy(
            mask_h.at[whole, halves[q]], MK.at[q], load_sem.at[24 + q]))
    for copy in loads:
        copy.start()

    barrier = pltpu.get_barrier_semaphore()
    for neighbour in (left, right):
        pl.semaphore_signal(barrier, inc=1, device_id={"gx": neighbour}, device_id_type=MESH_IDS)

    @pl.when(has_down)
    def _():
        pl.semaphore_signal(barrier, inc=1, device_id={"gy": gy - 1}, device_id_type=MESH_IDS)

    @pl.when(has_up)
    def _():
        pl.semaphore_signal(barrier, inc=1, device_id={"gy": gy + 1}, device_id_type=MESH_IDS)

    ens = lax.axis_index("ens")
    z_hi, y = ens // 4, lax.rem(ens, 4)
    y_peers = [z_hi * 4 + lax.rem(y + d, 4) for d in (1, 2, 3)]
    partner = (1 - z_hi) * 4 + y
    for peer in y_peers + [partner]:
        pl.semaphore_signal(barrier, inc=1, device_id={"ens": peer}, device_id_type=MESH_IDS)

    zero = jnp.zeros((8, LANES), jnp.float32)
    for f in (PP, MM, TT):
        for q in range(3):
            F[f, q, tile(0), :] = zero
    for f in (2, 3, 4):
        for q in range(3):
            RL[f, q, tile(0), :] = zero

    for copy in loads:
        copy.wait()

    def slot_mask(start, width):
        return lax.rem(lane - start + 2 * LANES, LANES) < width

    def derive(block, carry):
        present = []
        for q in range(2):
            c = [ice_s[0, block, 4 * q + n] for n in range(4)]
            present.append(jnp.where(
                lane < 64, jnp.where(lane < 32, c[0], c[1]), jnp.where(lane < 96, c[2], c[3])))
        for n in range(4):
            r = pl.multiple_of(block * 32 + 8 * n, 8)
            fields = []
            for q in range(2):
                u, v, s0, s1, s2, thick, conc, mass, we, wn, ce, cn = (
                    IN[f, q, tile(r), :] for f in range(12))
                active = (MK[q, tile(r), :] * present[q]).astype(jnp.float32)
                u, v = u * active, v * active
                strength = thick * jnp.exp(-DECAY * (1.0 - conc))
                s0, s2 = s0 * BETA, s2 * (2.0 * BETA)
                scale = 0.5 / ROOT2
                fields.append((
                    0.5 * (u + v), 0.5 * (u - v), s0 + s2, s0 - s2, s1 * BETA, strength * GAIN,
                    mass * ROOT2, scale * (we + wn), scale * (we - wn),
                    0.5 * (ce + cn), 0.5 * (ce - cn), active))
                for f in range(SENT):
                    F[f, q, tile(r + BASE), :] = fields[q][f]
            for part in range(2):
                to_left = to_right = None
                for s in range(6):
                    f = 6 * part + s
                    low = pltpu.roll(fields[0][f], PITCH * s, 1) if s else fields[0][f]
                    high = pltpu.roll(fields[1][f], (PITCH * s + 33) % LANES, 1)
                    if s == 0:
                        to_left, to_right = low, high
                    else:
                        to_left = jnp.where(slot_mask(PITCH * s, 17), low, to_left)
                        to_right = jnp.where(slot_mask(PITCH * s + 17, 16), high, to_right)
                SP[0, part, tile(r), :] = to_left
                SP[1, part, tile(r), :] = to_right
        return carry

    lax.fori_loop(0, ROWS // 32, derive, 0)

    pl.semaphore_wait(barrier, 6 + has_down.astype(jnp.int32) + has_up.astype(jnp.int32))

    to_left = pltpu.make_async_remote_copy(
        SP.at[0], RP.at[0], send_sem.at[0], recv_sem.at[0],
        device_id={"gx": left}, device_id_type=MESH_IDS)
    to_right = pltpu.make_async_remote_copy(
        SP.at[1], RP.at[1], send_sem.at[1], recv_sem.at[1],
        device_id={"gx": right}, device_id_type=MESH_IDS)
    to_left.start()
    to_right.start()

    def row_copies(q, count, n):
        planes = pl.ds(q, count)

        def part(f0, nf, src, dst, rows, slot, row):
            return pltpu.make_async_remote_copy(
                F.at[pl.ds(f0, nf), planes, pl.ds(src, rows)],
                F.at[pl.ds(f0, nf), planes, pl.ds(dst, rows)],
                send_sem.at[slot], recv_sem.at[slot],
                device_id={"gy": row}, device_id_type=MESH_IDS)

        down = [part(0, SENT, BASE, BASE + ROWS, HALO, n, gy - 1),
                part(0, 2, BASE + HALO, BASE + ROWS + HALO, 8, n + 1, gy - 1)]
        up = [part(0, SENT, BASE + ROWS - HALO, BASE - HALO, HALO, n + 2, gy + 1)]
        return down, up

    main_down, main_up = row_copies(0, 2, 2)
    strip_down, strip_up = row_copies(2, 1, 5)

    def start_rows(down, up):
        @pl.when(has_down)
        def _():
            for copy in down:
                copy.start()

        @pl.when(has_up)
        def _():
            for copy in up:
                copy.start()

    def wait_rows(down, up):
        @pl.when(has_down)
        def _():
            for copy in down:
                copy.wait_send()
            for copy in up:
                copy.wait_recv()

        @pl.when(has_up)
        def _():
            for copy in up:
                copy.wait_send()
            for copy in down:
                copy.wait_recv()

    start_rows(main_down, main_up)
    to_left.wait_recv()
    to_right.wait_recv()

    def build(block, carry):
        for n in range(2):
            r = pl.multiple_of(block * 16 + 8 * n, 8)
            for part in range(2):
                from_right, from_left = RP[0, part, tile(r), :], RP[1, part, tile(r), :]
                for s in range(6):
                    f = 6 * part + s
                    both = jnp.where(slot_mask(PITCH * s + 17, 16), from_left, from_right)
                    both = pltpu.roll(both, (95 - PITCH * s) % LANES, 1)
                    high = pltpu.roll(F[f, 1, tile(r + BASE), :], 95, 1)
                    F[f, 2, tile(r + BASE), :] = jnp.where(
                        lane < 48, F[f, 0, tile(r + BASE), :], jnp.where(lane < 95, high, both))
        return carry

    lax.fori_loop(0, ROWS // 16, build, 0)
    start_rows(strip_down, strip_up)

    def outside(start, count):
        for f in range(SENT):
            value = jnp.ones((8, LANES), jnp.float32) if f == MA else zero
            for q in range(3):
                for n in range(count):
                    F[f, q, tile(start + 8 * n), :] = value

    @pl.when(jnp.logical_not(has_down))
    def _():
        outside(BASE - HALO, 2)

    @pl.when(jnp.logical_not(has_up))
    def _():
        outside(BASE + ROWS, 3)

    to_left.wait_send()
    to_right.wait_send()
    wait_rows(main_down, main_up)
    wait_rows(strip_down, strip_up)

    sub = lax.broadcasted_iota(jnp.int32, (8, LANES), 0)
    grid_rows = ny * ROWS

    def prepare(t, carry):
        r = pl.multiple_of(8 * t, 8)
        row = (sub + (gy * ROWS - BASE + r)).astype(jnp.float32) + 0.5
        half = row * (0.5 / grid_rows)
        for q in range(3):
            b = half * F[MA, q, tile(r), :]
            F[BB, q, tile(r), :] = b
            F[B2, q, tile(r), :] = jnp.where(F[B2, q, tile(r), :] > 0.5, b * b, jnp.inf)
        return carry

    lax.fori_loop(FIRST, LAST, prepare, 0)

    def turn_first(t, carry):
        r = pl.multiple_of(8 * t, 8)
        for dst, f in ((0, W), (1, Z)):
            v = [pltpu.roll(F[f, q, tile(r), :], LANES - 1, 1) for q in range(3)]
            RL[dst, 0, tile(r), :] = jnp.where(lane == LANES - 1, v[1], v[0])
            RL[dst, 1, tile(r), :] = jnp.where(lane == LANES - 1, v[0], v[1])
            RL[dst, 2, tile(r), :] = v[2]
        return carry

    lax.fori_loop(FIRST, LAST + 1, turn_first, 0)

    whole_state, whole_rolled, const = (F, 0), (RL, 0), (F, 0)

    def main_cycle(n, carry):
        sweep(whole_state, whole_rolled, const, (0, 1), FIRST, LAST, LAG)
        return carry

    def strip_cycle(n, carry):
        sweep(whole_state, whole_rolled, const, (2,), FIRST, LAST, LAG)
        return carry

    lax.fori_loop(0, EARLY, main_cycle, 0)
    lax.fori_loop(0, EARLY, strip_cycle, 0)

    def merged(values):
        low = jnp.where(lane < 16, values[2], values[0])
        high = jnp.where(lane >= 108, pltpu.roll(values[2], 33, 1), values[1])
        return low, high

    def chunk_stores(i):
        rows = pl.ds(CHUNK * i, CHUNK)
        targets = [(FB.at[1], vel_o.at[0, 0]), (FB.at[2], vel_o.at[0, 1]), (OUT.at[0], st_o.at[0, 0]),
                   (OUT.at[1], st_o.at[0, 1]), (OUT.at[2], st_o.at[0, 2])]
        return [
            pltpu.make_async_copy(
                source.at[q, rows], target.at[rows, halves[q]], out_sem.at[10 * i + 2 * n + q])
            for n, (source, target) in enumerate(targets) for q in range(2)]

    def y_copy(i, d):
        target = lax.rem(y + d, 4)
        block = i // 2
        rows = pl.ds(pl.multiple_of(CHUNK * i + OWN * lax.rem(target, 2), 8), OWN)
        return target // 2 == i % 2, pltpu.make_async_remote_copy(
            FB.at[:, :, rows], YR.at[block, 3 - d],
            ysend_sem.at[3 * block + d - 1], yrecv_sem.at[3 * block + 3 - d],
            device_id={"ens": y_peers[d - 1]}, device_id_type=MESH_IDS)

    z_copy = pltpu.make_async_remote_copy(
        PART.at[1 - z_hi], ZR, zsend_sem, zrecv_sem,
        device_id={"ens": partner}, device_id_type=MESH_IDS)

    def partial(i):
        block = i // 2

        @pl.when(y // 2 == i % 2)
        def _():
            for d in (1, 2, 3):
                y_copy(i, d)[1].wait_recv()
            own = CHUNK * i + OWN * lax.rem(y, 2)

            def reduce(n, carry):
                r = pl.multiple_of(8 * n, 8)
                for f in range(3):
                    for q in range(2):
                        v = [YR[block, d, f, q, tile(r), :] for d in range(3)]
                        v.append(FB[f, q, tile(pl.multiple_of(own + r, 8)), :])
                        total = (v[0] + v[1]) + (v[2] + v[3])
                        mean = total * 0.25
                        e = [x - mean for x in v]
                        PART[block, 0, f, q, tile(r), :] = total
                        PART[block, 1, f, q, tile(r), :] = (
                            (e[0] * e[0] + e[1] * e[1]) + (e[2] * e[2] + e[3] * e[3]))
                return carry

            lax.fori_loop(0, OWN // 8, reduce, 0)

            @pl.when(z_hi != block)
            def _():
                z_copy.start()

    order = (0, 2, 1, 3)
    for place, i in enumerate(order):
        base = BASE - 16 + CHUNK * i

        def fetch(t, carry):
            r = pl.multiple_of(8 * t, 8)
            for q in range(3):
                for f in range(5):
                    G[f, q, tile(r), :] = F[f, q, tile(r + base), :]
                    G[5 + f, q, tile(r), :] = RL[f, q, tile(r + base), :]
            return carry

        lax.fori_loop(0, CTILES + 2, fetch, 0)

        def chunk_cycle(n, carry):
            sweep((G, 0), (G.at[pl.ds(5, 5)], 0), (F, base), (0, 1, 2), 1, CTILES + 1, CLAG)
            return carry

        lax.fori_loop(0, SUBCYCLES - EARLY, chunk_cycle, 0)

        def finish(n, carry):
            o = pl.multiple_of(8 * n + CHUNK * i, 8)
            r = pl.multiple_of(8 * n + 16, 8)
            div = []
            for q in range(3):
                a = G[5, q, tile(r + 1), :] - G[W, q, tile(r), :]
                b = G[6, q, tile(r), :] - G[Z, q, tile(r + 1), :]
                div.append(a + b)
            div = merged(div)
            w, z, p, m, t = (
                merged([G[f, q, tile(r), :] for q in range(3)]) for f in (W, Z, PP, MM, TT))
            for q in range(2):
                conc = IN[6, q, tile(o), :]
                FB[0, q, tile(o), :] = jnp.clip(conc - conc * div[q], 0.0, 1.0)
                FB[1, q, tile(o), :] = w[q] + z[q]
                FB[2, q, tile(o), :] = w[q] - z[q]
                OUT[0, q, tile(o), :] = (p[q] + m[q]) * (0.5 / BETA)
                OUT[1, q, tile(o), :] = t[q] * (1.0 / BETA)
                OUT[2, q, tile(o), :] = (p[q] - m[q]) * (0.25 / BETA)
            return carry

        lax.fori_loop(0, CHUNK // 8, finish, 0)
        for d in (1, 2, 3):
            wanted, copy = y_copy(i, d)
            pl.when(wanted)(copy.start)
        for copy in chunk_stores(i):
            copy.start()
        if place:
            partial(order[place - 1])
    partial(order[-1])

    z_copy.wait_recv()

    def combine(n, carry):
        r = pl.multiple_of(8 * n, 8)
        for f in range(3):
            for q in range(2):
                sa, sb = PART[z_hi, 0, f, q, tile(r), :], ZR[0, f, q, tile(r), :]
                ma, mb = PART[z_hi, 1, f, q, tile(r), :], ZR[1, f, q, tile(r), :]
                STAT[0, f, q, tile(r), :] = (sa + sb) * 0.125
                STAT[1, f, q, tile(r), :] = ((ma + mb) + (sa - sb) * (sa - sb) * 0.125) * 0.125
        return carry

    lax.fori_loop(0, OWN // 8, combine, 0)
    results = [
        pltpu.make_async_copy(
            STAT.at[n, :, q], target.at[:, :, halves[q]], out_sem.at[40 + 2 * n + q])
        for n, target in enumerate((mean_o, var_o)) for q in range(2)]
    for copy in results:
        copy.start()
    for i in order:
        for copy in chunk_stores(i):
            copy.wait()
        for d in (1, 2, 3):
            wanted, copy = y_copy(i, d)
            pl.when(wanted)(copy.wait_send)
    z_copy.wait_send()
    for copy in results:
        copy.wait()


def body(velocity, stress, thickness, concentration, node_mass, wind_stress, ocean_current,
         ocean_mask, ice_blocks):
    f32 = jnp.float32
    anywhere = pl.BlockSpec(memory_space=pl.ANY)
    stat = jax.ShapeDtypeStruct((3, OWN, 2 * LANES), f32)
    return pl.pallas_call(
        kernel,
        out_shape=(
            jax.ShapeDtypeStruct(velocity.shape, f32),
            jax.ShapeDtypeStruct(stress.shape, f32),
            stat,
            stat,
        ),
        in_specs=[anywhere] * 8 + [pl.BlockSpec(memory_space=pltpu.SMEM)],
        out_specs=(anywhere,) * 4,
        scratch_shapes=[
            pltpu.VMEM((13, 3, ALLOC, LANES), f32),
            pltpu.VMEM((5, 3, ALLOC, LANES), f32),
            pltpu.VMEM((12, 2, ROWS, LANES), f32),
            pltpu.VMEM((2, ROWS, LANES), jnp.int32),
            pltpu.VMEM((2, 2, ROWS, LANES), f32),
            pltpu.VMEM((2, 2, ROWS, LANES), f32),
            pltpu.VMEM((3, 2, ROWS, LANES), f32),
            pltpu.VMEM((10, 3, 8 * (CTILES + 2), LANES), f32),
            pltpu.VMEM((3, 2, ROWS, LANES), f32),
            pltpu.VMEM((2, 3, 3, 2, OWN, LANES), f32),
            pltpu.VMEM((2, 2, 3, 2, OWN, LANES), f32),
            pltpu.VMEM((2, 3, 2, OWN, LANES), f32),
            pltpu.VMEM((2, 3, 2, OWN, LANES), f32),
            pltpu.SemaphoreType.DMA((26,)),
            pltpu.SemaphoreType.DMA((8,)),
            pltpu.SemaphoreType.DMA((8,)),
            pltpu.SemaphoreType.DMA((44,)),
            pltpu.SemaphoreType.DMA((6,)),
            pltpu.SemaphoreType.DMA((6,)),
            pltpu.SemaphoreType.DMA,
            pltpu.SemaphoreType.DMA,
        ],
        compiler_params=pltpu.CompilerParams(
            collective_id=0, has_side_effects=True, vmem_limit_bytes=67043328),
        name="ice",
    )(velocity, stress, thickness, concentration, node_mass, wind_stress, ocean_current,
      ocean_mask, ice_blocks)


def solution(mesh):
    member, field = P("ens", None, "gy", "gx"), P("ens", "gy", "gx")
    placed = (member, member, field, field, field, member, member, P("gy", "gx"), field)
    block = P(None, ("gy", "ens"), "gx")
    return jax.shard_map(
        body, mesh=mesh, in_specs=placed, out_specs=(member, member, block, block),
        check_vma=False)
```

```python
import functools
import math

import jax
import jax.numpy as jnp
from jax import lax
from jax.experimental import pallas as pl
from jax.experimental.pallas import tpu as pltpu
from jax.sharding import PartitionSpec as P

SUBCYCLES = 16
RELAX = 0.25
DECAY = 20.0
FLOOR = 0.5
ROOT2 = math.sqrt(2.0)
BETA = 1.0 / (4.0 * ROOT2)
KEEP = 1.0 / (1.0 + RELAX)
GAIN = BETA * 0.5 * RELAX * KEEP
TINY = 1.1754944e-38

LANES = 128
ROWS = 256
BASE = 24
HALO = 16
ALLOC = 312
INNER, INNER_END = 3, 35
W, Z, PP, MM, TT, SM, MA, WW, WZ, CW, CZ, AC, BB, BS = range(14)
SENT = 12
PITCH = 20
LAG = 8
EARLY = 8
CHUNK = 64
CTILES = CHUNK // 8 + 2
CLAG = 3
OWN = 32
MESH_IDS = pl.DeviceIdType.MESH


def lane_ids():
    return lax.broadcasted_iota(jnp.int32, (8, LANES), 1)


def tile(r):
    return pl.ds(r, 8)


def sweep(state, rolled, const, tiles, first, last, lag):
    sweep_many([(state, rolled, const)], tiles, first, last, lag)


def sweep_many(regions, tiles, first, last, lag):
    steps = [updates(*region, tiles) for region in regions]
    for k in range(last - first + lag):
        for stress, momentum in steps:
            if first + k < last:
                stress(first + k)
        for stress, momentum in steps:
            if k >= lag:
                momentum(first + k - lag)


def updates(state, rolled, const, tiles):
    lane = lane_ids()
    low, high = lane == 0, lane == LANES - 1
    (S, so), (RL, ro), (C, co) = state, rolled, const

    def ld(f, q, r):
        return S[f, q, tile(r + so), :]

    def rl(f, q, r):
        return RL[f, q, tile(r + ro), :]

    def const_of(f, q, r):
        return C[f, q, tile(r + co), :]

    def turn(dst, src, t, shift, edge):
        values = [pltpu.roll(ld(src, q, 8 * t), shift, 1) for q in tiles]
        if len(tiles) > 1:
            values[:2] = [jnp.where(edge, values[1 - n], values[n]) for n in range(2)]
        for q, value in zip(tiles, values):
            RL[dst, q, tile(8 * t + ro), :] = value

    def stress(t):
        r = 8 * t
        for q in tiles:
            w, wd = ld(W, q, r), ld(W, q, r + 1)
            z, zd = ld(Z, q, r), ld(Z, q, r + 1)
            w1, w1d = rl(0, q, r), rl(0, q, r + 1)
            z1, z1d = rl(1, q, r), rl(1, q, r + 1)
            a, b, c, d = w1d - w, z1 - zd, z1d - z, w1 - wd
            div, shear, tension = a + b, a - b, c + d
            s4, t4 = shear * 0.25, tension * 0.25
            square = div * div + (shear * s4 + tension * t4)
            inverse = lax.rsqrt(jnp.maximum(square, TINY))
            e = div - square * inverse
            g = const_of(SM, q, r) * jnp.minimum(inverse, 1.0 / FLOOR)
            S[PP, q, tile(r + so), :] = ld(PP, q, r) * KEEP + g * (e + s4)
            S[MM, q, tile(r + so), :] = ld(MM, q, r) * KEEP + g * (e - s4)
            S[TT, q, tile(r + so), :] = ld(TT, q, r) * KEEP + g * t4
        for dst, src in ((2, PP), (3, MM), (4, TT)):
            turn(dst, src, t, 1, low)

    def momentum(t):
        r = 8 * t
        for q in tiles:
            fw = (ld(PP, q, r) - rl(2, q, r - 1)) + (ld(TT, q, r - 1) - rl(4, q, r))
            fz = (ld(TT, q, r) - rl(4, q, r - 1)) + (ld(MM, q, r - 1) - rl(3, q, r))
            w, z = ld(W, q, r), ld(Z, q, r)
            cw, cz = const_of(CW, q, r), const_of(CZ, q, r)
            dw, dz = cw - w, cz - z
            dq = dw * dw + dz * dz
            drag = dq * lax.rsqrt(jnp.maximum(dq, TINY))
            mass, b = const_of(MA, q, r), const_of(BB, q, r)
            a = mass + drag
            rw = (mass * w + drag * cw) + (fw + const_of(WW, q, r))
            rz = (mass * z + drag * cz) + (fz + const_of(WZ, q, r))
            root = lax.rsqrt(a * a + const_of(BS, q, r))
            quotient = root * root
            a, b = a * quotient, b * quotient
            S[W, q, tile(r + so), :] = a * rw - b * rz
            S[Z, q, tile(r + so), :] = a * rz + b * rw
        for dst, src in ((0, W), (1, Z)):
            turn(dst, src, t, LANES - 1, high)

    return stress, momentum


def kernel(
    vel_h, st_h, thick_h, conc_h, mass_h, wind_h, cur_h, mask_h, ice_s,
    FB, OUT, STAT,
    F, RL, WG, IN, MK, SP, RP, G, YR, PART, ZR,
    load_sem, send_sem, recv_sem, ysend_sem, yrecv_sem, zsend_sem, zrecv_sem,
):
    gx, gy, ens = lax.axis_index("gx"), lax.axis_index("gy"), lax.axis_index("ens")
    nx, ny = lax.axis_size("gx"), lax.axis_size("gy")
    left, right = lax.rem(gx + nx - 1, nx), lax.rem(gx + 1, nx)
    has_down, has_up = gy > 0, gy < ny - 1
    z_hi, y = ens // 4, lax.rem(ens, 4)
    y_peers = [z_hi * 4 + lax.rem(y + d, 4) for d in (1, 2, 3)]
    partner = (1 - z_hi) * 4 + y
    lane = lane_ids()
    zero = jnp.zeros((8, LANES), jnp.float32)

    sources = [vel_h.at[0, 0], vel_h.at[0, 1], st_h.at[0, 0], st_h.at[0, 1], st_h.at[0, 2],
               thick_h.at[0], conc_h.at[0], mass_h.at[0], wind_h.at[0, 0], wind_h.at[0, 1],
               cur_h.at[0, 0], cur_h.at[0, 1]]
    loads = []
    for q in range(2):
        columns = pl.ds(LANES * q, LANES)
        for n, source in enumerate(sources):
            loads.append(pltpu.make_async_copy(
                source.at[:, columns], IN.at[n, q], load_sem.at[2 * n + q]))
        loads.append(pltpu.make_async_copy(mask_h.at[:, columns], MK.at[q], load_sem.at[24 + q]))
    for copy in loads:
        copy.start()

    barrier = pltpu.get_barrier_semaphore()

    def greet(**where):
        pl.semaphore_signal(barrier, inc=1, device_id=where, device_id_type=MESH_IDS)

    greet(gx=left)
    greet(gx=right)
    pl.when(has_down)(lambda: greet(gy=gy - 1))
    pl.when(has_up)(lambda: greet(gy=gy + 1))
    for peer in y_peers + [partner]:
        greet(ens=peer)

    for q in range(3):
        for t in (1, 2, INNER_END, INNER_END + 1):
            for f in range(5):
                F[f, q, tile(8 * t), :] = zero
                RL[f, q, tile(8 * t), :] = zero
        for side in range(2):
            for f in range(10):
                WG[side, f, q, tile(0), :] = zero
        for f in (PP, MM, TT):
            WG[1, f, q, tile(40), :] = zero

    for copy in loads:
        copy.wait()

    def slot_mask(start, width):
        return lax.rem(lane - start + 2 * LANES, LANES) < width

    def derive(block, carry):
        present = []
        for q in range(2):
            c = [ice_s[0, block, 4 * q + n] for n in range(4)]
            present.append(jnp.where(
                lane < 64, jnp.where(lane < 32, c[0], c[1]), jnp.where(lane < 96, c[2], c[3])))
        for n in range(4):
            r = pl.multiple_of(block * 32 + 8 * n, 8)
            fields = []
            for q in range(2):
                u, v, s0, s1, s2, thick, conc, mass, we, wn, ce, cn = (
                    IN[f, q, tile(r), :] for f in range(12))
                active = (MK[q, tile(r), :] * present[q]).astype(jnp.float32)
                u, v = u * active, v * active
                strength = thick * jnp.exp(-DECAY * (1.0 - conc))
                s0, s2 = s0 * BETA, s2 * (2.0 * BETA)
                scale = 0.5 / ROOT2
                fields.append((
                    0.5 * (u + v), 0.5 * (u - v), s0 + s2, s0 - s2, s1 * BETA, strength * GAIN,
                    mass * ROOT2, scale * (we + wn), scale * (we - wn),
                    0.5 * (ce + cn), 0.5 * (ce - cn), active))
                for f in range(SENT):
                    F[f, q, tile(r + BASE), :] = fields[q][f]
            for part in range(2):
                to_left = to_right = None
                for s in range(6):
                    f = 6 * part + s
                    low = pltpu.roll(fields[0][f], PITCH * s, 1) if s else fields[0][f]
                    high = pltpu.roll(fields[1][f], (PITCH * s + 33) % LANES, 1)
                    if s == 0:
                        to_left, to_right = low, high
                    else:
                        to_left = jnp.where(slot_mask(PITCH * s, 17), low, to_left)
                        to_right = jnp.where(slot_mask(PITCH * s + 17, 16), high, to_right)
                SP[0, part, tile(r), :] = to_left
                SP[1, part, tile(r), :] = to_right
        return carry

    lax.fori_loop(0, ROWS // 32, derive, 0)

    def edges(planes):
        for q in planes:
            for f in range(5):
                for t in (3, 4, 5):
                    WG[0, f, q, tile(8 * t), :] = F[f, q, tile(8 * t), :]
                for t in (1, 2):
                    WG[1, f, q, tile(8 * t), :] = F[f, q, tile(8 * t + ROWS), :]

    edges((0, 1))
    pl.semaphore_wait(barrier, 6 + has_down.astype(jnp.int32) + has_up.astype(jnp.int32))

    to_left = pltpu.make_async_remote_copy(
        SP.at[0], RP.at[0], send_sem.at[0], recv_sem.at[0],
        device_id={"gx": left}, device_id_type=MESH_IDS)
    to_right = pltpu.make_async_remote_copy(
        SP.at[1], RP.at[1], send_sem.at[1], recv_sem.at[1],
        device_id={"gx": right}, device_id_type=MESH_IDS)
    to_left.start()
    to_right.start()

    def row_copies(q, count, n):
        planes = pl.ds(q, count)

        def state(side, f0, nf, t, tiles, slot, row):
            rows = pl.ds(8 * t, 8 * tiles)
            return pltpu.make_async_remote_copy(
                WG.at[side, pl.ds(f0, nf), planes, rows],
                WG.at[1 - side, pl.ds(f0, nf), planes, rows],
                send_sem.at[slot], recv_sem.at[slot],
                device_id={"gy": row}, device_id_type=MESH_IDS)

        def given(src, dst, slot, row):
            return pltpu.make_async_remote_copy(
                F.at[pl.ds(5, SENT - 5), planes, pl.ds(src, HALO)],
                F.at[pl.ds(5, SENT - 5), planes, pl.ds(dst, HALO)],
                send_sem.at[slot], recv_sem.at[slot],
                device_id={"gy": row}, device_id_type=MESH_IDS)

        down = [state(0, 0, 2, 3, 3, n, gy - 1), state(0, 2, 3, 3, 2, n + 1, gy - 1),
                given(BASE, BASE + ROWS, n + 2, gy - 1)]
        up = [state(1, 0, 5, 1, 2, n + 3, gy + 1),
              given(BASE + ROWS - HALO, BASE - HALO, n + 4, gy + 1)]
        return down, up

    main_down, main_up = row_copies(0, 2, 2)
    strip_down, strip_up = row_copies(2, 1, 7)

    def start_rows(down, up):
        @pl.when(has_down)
        def _():
            for copy in down:
                copy.start()

        @pl.when(has_up)
        def _():
            for copy in up:
                copy.start()

    def wait_rows(down, up):
        @pl.when(has_down)
        def _():
            for copy in down:
                copy.wait_send()
            for copy in up:
                copy.wait_recv()

        @pl.when(has_up)
        def _():
            for copy in up:
                copy.wait_send()
            for copy in down:
                copy.wait_recv()

    start_rows(main_down, main_up)

    sub = lax.broadcasted_iota(jnp.int32, (8, LANES), 0)
    grid_rows = ny * ROWS

    def coriolis(t, planes):
        r = 8 * t if isinstance(t, int) else pl.multiple_of(8 * t, 8)
        row = (sub + (gy * ROWS - BASE + r)).astype(jnp.float32) + 0.5
        half = row * (0.5 / grid_rows)
        for q in planes:
            b = half * F[MA, q, tile(r), :]
            F[BB, q, tile(r), :] = b
            F[BS, q, tile(r), :] = jnp.where(F[AC, q, tile(r), :] > 0.5, b * b, jnp.inf)

    def first_turn(t, planes):
        r = pl.multiple_of(8 * t, 8)
        for dst, f in ((0, W), (1, Z)):
            v = [pltpu.roll(F[f, q, tile(r), :], LANES - 1, 1) for q in planes]
            if len(v) == 2:
                v = [jnp.where(lane == LANES - 1, v[1 - n], v[n]) for n in range(2)]
            for q, value in zip(planes, v):
                RL[dst, q, tile(r), :] = value

    def ready(planes):
        def body(n, carry):
            for k in range(8):
                coriolis(INNER + 8 * n + k, planes)
                first_turn(INNER + 8 * n + k, planes)
            return carry

        lax.fori_loop(0, (INNER_END - INNER) // 8, body, 0)

    whole_state, whole_rolled, const = (F, 0), (RL, 0), (F, 0)

    def inner_cycles(planes):
        def cycle(n, carry):
            sweep(whole_state, whole_rolled, const, planes, INNER, INNER_END, LAG)
            return carry

        lax.fori_loop(0, EARLY, cycle, 0)

    ready((0, 1))
    def build(block, carry):
        for n in range(4):
            r = pl.multiple_of(block * 32 + 8 * n, 8)
            for f in range(SENT):
                high = pltpu.roll(F[f, 1, tile(r + BASE), :], 95, 1)
                F[f, 2, tile(r + BASE), :] = jnp.where(
                    lane < 48, F[f, 0, tile(r + BASE), :], high)
        return carry

    lax.fori_loop(0, ROWS // 32, build, 0)
    inner_cycles((0, 1))

    to_left.wait_recv()
    to_right.wait_recv()

    def fill(block, carry):
        for n in range(4):
            r = pl.multiple_of(block * 32 + 8 * n, 8)
            for part in range(2):
                from_right, from_left = RP[0, part, tile(r), :], RP[1, part, tile(r), :]
                for s in range(6):
                    f = 6 * part + s
                    both = jnp.where(slot_mask(PITCH * s + 17, 16), from_left, from_right)
                    both = pltpu.roll(both, (95 - PITCH * s) % LANES, 1)
                    F[f, 2, tile(r + BASE), :] = jnp.where(
                        lane < 95, F[f, 2, tile(r + BASE), :], both)
        return carry

    lax.fori_loop(0, ROWS // 32, fill, 0)
    edges((2,))
    start_rows(strip_down, strip_up)
    ready((2,))
    inner_cycles((2,))

    to_left.wait_send()
    to_right.wait_send()
    wait_rows(main_down, main_up)
    wait_rows(strip_down, strip_up)

    def outside(side, tiles):
        for q in range(3):
            for t in tiles:
                for f in range(5):
                    WG[side, f, q, tile(8 * t), :] = zero
                if t < 5:
                    for f in range(5, SENT):
                        F[f, q, tile(8 * t + ROWS * side), :] = (
                            jnp.ones((8, LANES), jnp.float32) if f == MA else zero)

    pl.when(jnp.logical_not(has_down))(lambda: outside(0, (1, 2)))
    pl.when(jnp.logical_not(has_up))(lambda: outside(1, (3, 4, 5)))
    for t in (1, 2, INNER_END, INNER_END + 1):
        coriolis(t, (0, 1, 2))

    for side in range(2):
        for t in (1, 2, 3, 4, 5):
            for dst, f in ((5, W), (6, Z)):
                v = [pltpu.roll(WG[side, f, q, tile(8 * t), :], LANES - 1, 1) for q in range(3)]
                v[:2] = [jnp.where(lane == LANES - 1, v[1 - n], v[n]) for n in range(2)]
                for q in range(3):
                    WG[side, dst, q, tile(8 * t), :] = v[q]

    def wedge_cycle(n, carry):
        sweep_many(
            [((WG.at[side, pl.ds(0, 5)], 0), (WG.at[side, pl.ds(5, 5)], 0), (F, ROWS * side))
             for side in range(2)], (0, 1, 2), 1, 5, 2)
        return carry

    lax.fori_loop(0, EARLY, wedge_cycle, 0)
    for side, tiles in ((0, (2, 3)), (1, (2, 3, 4))):
        for t in tiles:
            for q in range(3):
                for f in range(5):
                    F[f, q, tile(8 * t + ROWS * side), :] = WG[side, f, q, tile(8 * t), :]
                    if f < 2:
                        RL[f, q, tile(8 * t + ROWS * side), :] = WG[side, 5 + f, q, tile(8 * t), :]

    def merged(values):
        low = jnp.where(lane < 16, values[2], values[0])
        high = jnp.where(lane >= 108, pltpu.roll(values[2], 33, 1), values[1])
        return low, high

    def y_copy(i, d):
        target = lax.rem(y + d, 4)
        block = i // 2
        rows = pl.ds(pl.multiple_of(CHUNK * i + OWN * lax.rem(target, 2), 8), OWN)
        return target // 2 == i % 2, pltpu.make_async_remote_copy(
            FB.at[:, :, rows], YR.at[block, 3 - d],
            ysend_sem.at[3 * block + d - 1], yrecv_sem.at[3 * block + 3 - d],
            device_id={"ens": y_peers[d - 1]}, device_id_type=MESH_IDS)

    z_copy = pltpu.make_async_remote_copy(
        PART.at[1 - z_hi], ZR, zsend_sem, zrecv_sem,
        device_id={"ens": partner}, device_id_type=MESH_IDS)

    def partial(i):
        block = i // 2

        @pl.when(y // 2 == i % 2)
        def _():
            for d in (1, 2, 3):
                y_copy(i, d)[1].wait_recv()
            own = CHUNK * i + OWN * lax.rem(y, 2)

            def reduce(n, carry):
                r = pl.multiple_of(8 * n, 8)
                for f in range(3):
                    for q in range(2):
                        v = [YR[block, d, f, q, tile(r), :] for d in range(3)]
                        v.append(FB[f, q, tile(pl.multiple_of(own + r, 8)), :])
                        total = (v[0] + v[1]) + (v[2] + v[3])
                        mean = total * 0.25
                        e = [x - mean for x in v]
                        PART[block, 0, f, q, tile(r), :] = total
                        PART[block, 1, f, q, tile(r), :] = (
                            (e[0] * e[0] + e[1] * e[1]) + (e[2] * e[2] + e[3] * e[3]))
                return carry

            lax.fori_loop(0, OWN // 8, reduce, 0)
            pl.when(z_hi != block)(z_copy.start)

    order = (0, 2, 1, 3)
    for place, i in enumerate(order):
        base = BASE - 16 + CHUNK * i

        def fetch(t, carry):
            r = pl.multiple_of(8 * t, 8)
            for q in range(3):
                for f in range(5):
                    G[f, q, tile(r), :] = F[f, q, tile(r + base), :]
                    G[5 + f, q, tile(r), :] = RL[f, q, tile(r + base), :]
            return carry

        lax.fori_loop(0, CTILES + 2, fetch, 0)

        def chunk_cycle(n, carry):
            sweep((G.at[pl.ds(0, 5)], 0), (G.at[pl.ds(5, 5)], 0), (F, base), (0, 1, 2), 1,
                  CTILES + 1, CLAG)
            return carry

        lax.fori_loop(0, SUBCYCLES - EARLY, chunk_cycle, 0)

        for n in range(CHUNK // 8):
            o, r = 8 * n + CHUNK * i, 8 * n + 16
            div = []
            for q in range(3):
                a = G[5, q, tile(r + 1), :] - G[W, q, tile(r), :]
                b = G[6, q, tile(r), :] - G[Z, q, tile(r + 1), :]
                div.append(a + b)
            div = merged(div)
            w, z, p, m, t = (
                merged([G[f, q, tile(r), :] for q in range(3)]) for f in (W, Z, PP, MM, TT))
            for q in range(2):
                conc = IN[6, q, tile(o), :]
                FB[0, q, tile(o), :] = jnp.clip(conc - conc * div[q], 0.0, 1.0)
                FB[1, q, tile(o), :] = w[q] + z[q]
                FB[2, q, tile(o), :] = w[q] - z[q]
                OUT[0, q, tile(o), :] = (p[q] + m[q]) * (0.5 / BETA)
                OUT[1, q, tile(o), :] = t[q] * (1.0 / BETA)
                OUT[2, q, tile(o), :] = (p[q] - m[q]) * (0.25 / BETA)
        for d in (1, 2, 3):
            wanted, copy = y_copy(i, d)
            pl.when(wanted)(copy.start)
        if place:
            partial(order[place - 1])
    partial(order[-1])

    z_copy.wait_recv()
    for n in range(OWN // 8):
        r = 8 * n
        for f in range(3):
            for q in range(2):
                sa, sb = PART[z_hi, 0, f, q, tile(r), :], ZR[0, f, q, tile(r), :]
                ma, mb = PART[z_hi, 1, f, q, tile(r), :], ZR[1, f, q, tile(r), :]
                STAT[0, f, q, tile(r), :] = (sa + sb) * 0.125
                STAT[1, f, q, tile(r), :] = ((ma + mb) + (sa - sb) * (sa - sb) * 0.125) * 0.125
    for i in order:
        for d in (1, 2, 3):
            wanted, copy = y_copy(i, d)
            pl.when(wanted)(copy.wait_send)
    z_copy.wait_send()


def emit(FB, OUT, STAT, vel_o, st_o, mean_o, var_o, sem):
    copies = []
    for q in range(2):
        columns = pl.ds(LANES * q, LANES)
        pairs = [(OUT.at[n, q], st_o.at[0, n]) for n in range(3)]
        pairs += [(FB.at[1 + n, q], vel_o.at[0, n]) for n in range(2)]
        for source, target in pairs:
            copies.append((source, target.at[:, columns]))
        for n, target in enumerate((mean_o, var_o)):
            copies.append((STAT.at[n, :, q], target.at[:, :, columns]))
    copies = [pltpu.make_async_copy(a, b, sem.at[n]) for n, (a, b) in enumerate(copies)]
    for copy in copies:
        copy.start()
    for copy in copies:
        copy.wait()


def body(velocity, stress, thickness, concentration, node_mass, wind_stress, ocean_current,
         ocean_mask, ice_blocks):
    f32 = jnp.float32
    hbm = pl.BlockSpec(memory_space=pltpu.HBM)
    vmem = pl.BlockSpec(memory_space=pltpu.VMEM)
    stat = jax.ShapeDtypeStruct((3, OWN, 2 * LANES), f32)
    big = [pltpu.with_memory_space_constraint(x, pltpu.HBM) for x in (velocity, stress, thickness, concentration, node_mass, wind_stress, ocean_current, ocean_mask)]
    results = pl.pallas_call(
        kernel,
        out_shape=(
            jax.ShapeDtypeStruct((3, 2, ROWS, LANES), f32),
            jax.ShapeDtypeStruct((3, 2, ROWS, LANES), f32),
            jax.ShapeDtypeStruct((2, 3, 2, OWN, LANES), f32),
        ),
        in_specs=[hbm] * 8 + [pl.BlockSpec(memory_space=pltpu.SMEM)],
        out_specs=(vmem,) * 3,
        scratch_shapes=[
            pltpu.VMEM((14, 3, ALLOC, LANES), f32),
            pltpu.VMEM((5, 3, ALLOC, LANES), f32),
            pltpu.VMEM((2, 10, 3, 48, LANES), f32),
            pltpu.VMEM((12, 2, ROWS, LANES), f32),
            pltpu.VMEM((2, ROWS, LANES), jnp.int32),
            pltpu.VMEM((2, 2, ROWS, LANES), f32),
            pltpu.VMEM((2, 2, ROWS, LANES), f32),
            pltpu.VMEM((10, 3, 8 * (CTILES + 2), LANES), f32),
            pltpu.VMEM((2, 3, 3, 2, OWN, LANES), f32),
            pltpu.VMEM((2, 2, 3, 2, OWN, LANES), f32),
            pltpu.VMEM((2, 3, 2, OWN, LANES), f32),
            pltpu.SemaphoreType.DMA((26,)),
            pltpu.SemaphoreType.DMA((12,)),
            pltpu.SemaphoreType.DMA((12,)),
            pltpu.SemaphoreType.DMA((6,)),
            pltpu.SemaphoreType.DMA((6,)),
            pltpu.SemaphoreType.DMA,
            pltpu.SemaphoreType.DMA,
        ],
        compiler_params=pltpu.CompilerParams(
            collective_id=0, has_side_effects=True, vmem_limit_bytes=40 * 1024 * 1024),
        name="ice",
    )(*big,
      ice_blocks)
    return pl.pallas_call(
        emit,
        out_shape=(
            jax.ShapeDtypeStruct(velocity.shape, f32),
            jax.ShapeDtypeStruct(stress.shape, f32),
            stat,
            stat,
        ),
        in_specs=[vmem] * 3,
        out_specs=(hbm,) * 4,
        scratch_shapes=[pltpu.SemaphoreType.DMA((14,))],
        compiler_params=pltpu.CompilerParams(vmem_limit_bytes=8 * 1024 * 1024),
        name="emit",
    )(*results)


def solution(mesh):
    member, field = P("ens", None, "gy", "gx"), P("ens", "gy", "gx")
    placed = (member, member, field, field, field, member, member, P("gy", "gx"), field)
    block = P(None, ("gy", "ens"), "gx")
    return jax.shard_map(
        body, mesh=mesh, in_specs=placed, out_specs=(member, member, block, block),
        check_vma=False)
```

```python
import functools
import math

import jax
import jax.numpy as jnp
from jax import lax
from jax.experimental import pallas as pl
from jax.experimental.pallas import tpu as pltpu
from jax.sharding import PartitionSpec as P

SUBCYCLES = 16
RELAX = 0.25
DECAY = 20.0
FLOOR = 0.5
ROOT2 = math.sqrt(2.0)
BETA = 1.0 / (4.0 * ROOT2)
KEEP = 1.0 / (1.0 + RELAX)
GAIN = BETA * 0.5 * RELAX * KEEP
TINY = 1.1754944e-38

LANES = 128
ROWS = 256
BASE = 24
HALO = 16
ALLOC = 312
INNER, INNER_END = 3, 35
W, Z, PP, MM, TT, SM, MA, WW, WZ, CW, CZ, AC, BB, BS = range(14)
SENT = 12
PITCH = 20
LAG = 8
EARLY = 8
GROWS = 12
CLAG = 3
OWN = 32
MESH_IDS = pl.DeviceIdType.MESH


def lane_ids():
    return lax.broadcasted_iota(jnp.int32, (8, LANES), 1)


def tile(r):
    return pl.ds(r, 8)


def sweep(state, rolled, const, tiles, first, last, lag):
    sweep_many([(state, rolled, const)], tiles, first, last, lag)


def sweep_many(regions, tiles, first, last, lag):
    steps = [updates(*region, tiles) for region in regions]
    for k in range(last - first + lag):
        for stress, momentum in steps:
            if first + k < last:
                stress(first + k)
        for stress, momentum in steps:
            if k >= lag:
                momentum(first + k - lag)


def updates(state, rolled, const, tiles):
    lane = lane_ids()
    low, high = lane == 0, lane == LANES - 1
    (S, so), (RL, ro), (C, co) = state, rolled, const

    def ld(f, q, r):
        return S[f, q, tile(r + so), :]

    def rl(f, q, r):
        return RL[f, q, tile(r + ro), :]

    def const_of(f, q, r):
        return C[f, q, tile(r + co), :]

    def turn(dst, src, t, shift, edge):
        values = [pltpu.roll(ld(src, q, 8 * t), shift, 1) for q in tiles]
        if len(tiles) > 1:
            values[:2] = [jnp.where(edge, values[1 - n], values[n]) for n in range(2)]
        for q, value in zip(tiles, values):
            RL[dst, q, tile(8 * t + ro), :] = value

    def stress(t):
        r = 8 * t
        for q in tiles:
            w, wd = ld(W, q, r), ld(W, q, r + 1)
            z, zd = ld(Z, q, r), ld(Z, q, r + 1)
            w1, w1d = rl(0, q, r), rl(0, q, r + 1)
            z1, z1d = rl(1, q, r), rl(1, q, r + 1)
            a, b, c, d = w1d - w, z1 - zd, z1d - z, w1 - wd
            div, shear, tension = a + b, a - b, c + d
            s4, t4 = shear * 0.25, tension * 0.25
            square = div * div + (shear * s4 + tension * t4)
            inverse = lax.rsqrt(jnp.maximum(square, TINY))
            e = div - square * inverse
            g = const_of(SM, q, r) * jnp.minimum(inverse, 1.0 / FLOOR)
            S[PP, q, tile(r + so), :] = ld(PP, q, r) * KEEP + g * (e + s4)
            S[MM, q, tile(r + so), :] = ld(MM, q, r) * KEEP + g * (e - s4)
            S[TT, q, tile(r + so), :] = ld(TT, q, r) * KEEP + g * t4
        for dst, src in ((2, PP), (3, MM), (4, TT)):
            turn(dst, src, t, 1, low)

    def momentum(t):
        r = 8 * t
        for q in tiles:
            fw = (ld(PP, q, r) - rl(2, q, r - 1)) + (ld(TT, q, r - 1) - rl(4, q, r))
            fz = (ld(TT, q, r) - rl(4, q, r - 1)) + (ld(MM, q, r - 1) - rl(3, q, r))
            w, z = ld(W, q, r), ld(Z, q, r)
            cw, cz = const_of(CW, q, r), const_of(CZ, q, r)
            dw, dz = cw - w, cz - z
            dq = dw * dw + dz * dz
            drag = dq * lax.rsqrt(jnp.maximum(dq, TINY))
            mass, b = const_of(MA, q, r), const_of(BB, q, r)
            a = mass + drag
            rw = (mass * w + drag * cw) + (fw + const_of(WW, q, r))
            rz = (mass * z + drag * cz) + (fz + const_of(WZ, q, r))
            root = lax.rsqrt(a * a + const_of(BS, q, r))
            quotient = root * root
            a, b = a * quotient, b * quotient
            S[W, q, tile(r + so), :] = a * rw - b * rz
            S[Z, q, tile(r + so), :] = a * rz + b * rw
        for dst, src in ((0, W), (1, Z)):
            turn(dst, src, t, LANES - 1, high)

    return stress, momentum


def kernel(
    vel_h, st_h, thick_h, conc_h, mass_h, wind_h, cur_h, mask_h, ice_h,
    FB, OUT, STAT,
    F, RL, WG, IN, MK, SP, RP, G, YR, PART, ZR, ice_s,
    load_sem, ice_sem, send_sem, recv_sem, ysend_sem, yrecv_sem, zsend_sem, zrecv_sem,
):
    gx, gy, ens = lax.axis_index("gx"), lax.axis_index("gy"), lax.axis_index("ens")
    nx, ny = lax.axis_size("gx"), lax.axis_size("gy")
    left, right = lax.rem(gx + nx - 1, nx), lax.rem(gx + 1, nx)
    has_down, has_up = gy > 0, gy < ny - 1
    z_hi, y = ens // 4, lax.rem(ens, 4)
    y_peers = [z_hi * 4 + lax.rem(y + d, 4) for d in (1, 2, 3)]
    lane = lane_ids()
    zero = jnp.zeros((8, LANES), jnp.float32)

    sources = [vel_h.at[0, 0], vel_h.at[0, 1], st_h.at[0, 0], st_h.at[0, 1], st_h.at[0, 2],
               thick_h.at[0], conc_h.at[0], mass_h.at[0], wind_h.at[0, 0], wind_h.at[0, 1],
               cur_h.at[0, 0], cur_h.at[0, 1]]
    ice_load = pltpu.make_async_copy(ice_h, ice_s, ice_sem)
    ice_load.start()
    loads = [[], []]
    for half in range(2):
        rows = pl.ds(ROWS // 2 * half, ROWS // 2)
        for q in range(2):
            columns = pl.ds(LANES * q, LANES)
            places = [IN.at[n, q, rows] for n in range(12)] + [MK.at[q, rows]]
            for n, (source, place) in enumerate(zip(sources + [mask_h], places)):
                loads[half].append(pltpu.make_async_copy(
                    source.at[rows, columns], place, load_sem.at[26 * half + 13 * q + n]))
    for copy in loads[0] + loads[1]:
        copy.start()

    barrier = pltpu.get_barrier_semaphore()

    def greet(**where):
        pl.semaphore_signal(barrier, inc=1, device_id=where, device_id_type=MESH_IDS)

    greet(gx=left)
    greet(gx=right)
    pl.when(has_down)(lambda: greet(gy=gy - 1))
    pl.when(has_up)(lambda: greet(gy=gy + 1))
    for d in range(1, 8):
        greet(ens=lax.rem(ens + d, 8))

    for q in range(3):
        for t in (1, 2, INNER_END, INNER_END + 1):
            for f in range(5):
                F[f, q, tile(8 * t), :] = zero
                RL[f, q, tile(8 * t), :] = zero
        for side in range(2):
            for f in range(10):
                WG[side, f, q, tile(0), :] = zero
        for f in (PP, MM, TT):
            WG[1, f, q, tile(40), :] = zero

    def slot_mask(start, width):
        return lax.rem(lane - start + 2 * LANES, LANES) < width

    def derive(block, carry):
        present = []
        for q in range(2):
            c = [ice_s[0, block, 4 * q + n] for n in range(4)]
            present.append(jnp.where(
                lane < 64, jnp.where(lane < 32, c[0], c[1]), jnp.where(lane < 96, c[2], c[3])))
        for n in range(4):
            r = pl.multiple_of(block * 32 + 8 * n, 8)
            fields = []
            for q in range(2):
                u, v, s0, s1, s2, thick, conc, mass, we, wn, ce, cn = (
                    IN[f, q, tile(r), :] for f in range(12))
                active = (MK[q, tile(r), :] * present[q]).astype(jnp.float32)
                u, v = u * active, v * active
                strength = thick * jnp.exp(-DECAY * (1.0 - conc))
                s0, s2 = s0 * BETA, s2 * (2.0 * BETA)
                scale = 0.5 / ROOT2
                fields.append((
                    0.5 * (u + v), 0.5 * (u - v), s0 + s2, s0 - s2, s1 * BETA, strength * GAIN,
                    mass * ROOT2, scale * (we + wn), scale * (we - wn),
                    0.5 * (ce + cn), 0.5 * (ce - cn), active))
                for f in range(SENT):
                    F[f, q, tile(r + BASE), :] = fields[q][f]
            for part in range(2):
                to_left = to_right = None
                for s in range(6):
                    f = 6 * part + s
                    low = pltpu.roll(fields[0][f], PITCH * s, 1) if s else fields[0][f]
                    high = pltpu.roll(fields[1][f], (PITCH * s + 33) % LANES, 1)
                    if s == 0:
                        to_left, to_right = low, high
                    else:
                        to_left = jnp.where(slot_mask(PITCH * s, 17), low, to_left)
                        to_right = jnp.where(slot_mask(PITCH * s + 17, 16), high, to_right)
                SP[0, part, tile(r), :] = to_left
                SP[1, part, tile(r), :] = to_right
        return carry

    ice_load.wait()
    for half in range(2):
        for copy in loads[half]:
            copy.wait()
        lax.fori_loop(4 * half, 4 * half + 4, derive, 0)

    def edges(planes):
        for q in planes:
            for f in range(5):
                for t in (3, 4, 5):
                    WG[0, f, q, tile(8 * t), :] = F[f, q, tile(8 * t), :]
                for t in (1, 2):
                    WG[1, f, q, tile(8 * t), :] = F[f, q, tile(8 * t + ROWS), :]

    edges((0, 1))
    pl.semaphore_wait(barrier, 9 + has_down.astype(jnp.int32) + has_up.astype(jnp.int32))

    to_left = pltpu.make_async_remote_copy(
        SP.at[0], RP.at[0], send_sem.at[0], recv_sem.at[0],
        device_id={"gx": left}, device_id_type=MESH_IDS)
    to_right = pltpu.make_async_remote_copy(
        SP.at[1], RP.at[1], send_sem.at[1], recv_sem.at[1],
        device_id={"gx": right}, device_id_type=MESH_IDS)
    to_left.start()
    to_right.start()

    def row_copies(q, count, n):
        planes = pl.ds(q, count)

        def state(side, f0, nf, t, tiles, slot, row):
            rows = pl.ds(8 * t, 8 * tiles)
            return pltpu.make_async_remote_copy(
                WG.at[side, pl.ds(f0, nf), planes, rows],
                WG.at[1 - side, pl.ds(f0, nf), planes, rows],
                send_sem.at[slot], recv_sem.at[slot],
                device_id={"gy": row}, device_id_type=MESH_IDS)

        def given(src, dst, slot, row):
            return pltpu.make_async_remote_copy(
                F.at[pl.ds(5, SENT - 5), planes, pl.ds(src, HALO)],
                F.at[pl.ds(5, SENT - 5), planes, pl.ds(dst, HALO)],
                send_sem.at[slot], recv_sem.at[slot],
                device_id={"gy": row}, device_id_type=MESH_IDS)

        down = [state(0, 0, 2, 3, 3, n, gy - 1), state(0, 2, 3, 3, 2, n + 1, gy - 1),
                given(BASE, BASE + ROWS, n + 2, gy - 1)]
        up = [state(1, 0, 5, 1, 2, n + 3, gy + 1),
              given(BASE + ROWS - HALO, BASE - HALO, n + 4, gy + 1)]
        return down, up

    main_down, main_up = row_copies(0, 2, 2)
    strip_down, strip_up = row_copies(2, 1, 7)

    def start_rows(down, up):
        @pl.when(has_down)
        def _():
            for copy in down:
                copy.start()

        @pl.when(has_up)
        def _():
            for copy in up:
                copy.start()

    def wait_rows(down, up):
        @pl.when(has_down)
        def _():
            for copy in down:
                copy.wait_send()
            for copy in up:
                copy.wait_recv()

        @pl.when(has_up)
        def _():
            for copy in up:
                copy.wait_send()
            for copy in down:
                copy.wait_recv()

    start_rows(main_down, main_up)

    sub = lax.broadcasted_iota(jnp.int32, (8, LANES), 0)
    grid_rows = ny * ROWS

    def coriolis(t, planes):
        r = 8 * t if isinstance(t, int) else pl.multiple_of(8 * t, 8)
        row = (sub + (gy * ROWS - BASE + r)).astype(jnp.float32) + 0.5
        half = row * (0.5 / grid_rows)
        for q in planes:
            b = half * F[MA, q, tile(r), :]
            F[BB, q, tile(r), :] = b
            F[BS, q, tile(r), :] = jnp.where(F[AC, q, tile(r), :] > 0.5, b * b, jnp.inf)

    def first_turn(t, planes):
        r = pl.multiple_of(8 * t, 8)
        for dst, f in ((0, W), (1, Z)):
            v = [pltpu.roll(F[f, q, tile(r), :], LANES - 1, 1) for q in planes]
            if len(v) == 2:
                v = [jnp.where(lane == LANES - 1, v[1 - n], v[n]) for n in range(2)]
            for q, value in zip(planes, v):
                RL[dst, q, tile(r), :] = value

    def ready(planes):
        def body(n, carry):
            for k in range(8):
                coriolis(INNER + 8 * n + k, planes)
                first_turn(INNER + 8 * n + k, planes)
            return carry

        lax.fori_loop(0, (INNER_END - INNER) // 8, body, 0)

    whole_state, whole_rolled, const = (F, 0), (RL, 0), (F, 0)

    def inner_cycles(planes):
        def cycle(n, carry):
            sweep(whole_state, whole_rolled, const, planes, INNER, INNER_END, LAG)
            return carry

        lax.fori_loop(0, EARLY, cycle, 0)

    ready((0, 1))
    def build(block, carry):
        for n in range(4):
            r = pl.multiple_of(block * 32 + 8 * n, 8)
            for f in range(SENT):
                high = pltpu.roll(F[f, 1, tile(r + BASE), :], 95, 1)
                F[f, 2, tile(r + BASE), :] = jnp.where(
                    lane < 48, F[f, 0, tile(r + BASE), :], high)
        return carry

    lax.fori_loop(0, ROWS // 32, build, 0)
    inner_cycles((0, 1))

    to_left.wait_recv()
    to_right.wait_recv()

    def fill(block, carry):
        for n in range(4):
            r = pl.multiple_of(block * 32 + 8 * n, 8)
            for part in range(2):
                from_right, from_left = RP[0, part, tile(r), :], RP[1, part, tile(r), :]
                for s in range(6):
                    f = 6 * part + s
                    both = jnp.where(slot_mask(PITCH * s + 17, 16), from_left, from_right)
                    both = pltpu.roll(both, (95 - PITCH * s) % LANES, 1)
                    F[f, 2, tile(r + BASE), :] = jnp.where(
                        lane < 95, F[f, 2, tile(r + BASE), :], both)
        return carry

    lax.fori_loop(0, ROWS // 32, fill, 0)
    edges((2,))
    start_rows(strip_down, strip_up)
    ready((2,))
    inner_cycles((2,))

    to_left.wait_send()
    to_right.wait_send()
    wait_rows(main_down, main_up)
    wait_rows(strip_down, strip_up)

    def outside(side, tiles):
        for q in range(3):
            for t in tiles:
                for f in range(5):
                    WG[side, f, q, tile(8 * t), :] = zero
                if t < 5:
                    for f in range(5, SENT):
                        F[f, q, tile(8 * t + ROWS * side), :] = (
                            jnp.ones((8, LANES), jnp.float32) if f == MA else zero)

    pl.when(jnp.logical_not(has_down))(lambda: outside(0, (1, 2)))
    pl.when(jnp.logical_not(has_up))(lambda: outside(1, (3, 4, 5)))
    for t in (1, 2, INNER_END, INNER_END + 1):
        coriolis(t, (0, 1, 2))

    for side in range(2):
        for t in (1, 2, 3, 4, 5):
            for dst, f in ((5, W), (6, Z)):
                v = [pltpu.roll(WG[side, f, q, tile(8 * t), :], LANES - 1, 1) for q in range(3)]
                v[:2] = [jnp.where(lane == LANES - 1, v[1 - n], v[n]) for n in range(2)]
                for q in range(3):
                    WG[side, dst, q, tile(8 * t), :] = v[q]

    def wedge_cycle(n, carry):
        sweep_many(
            [((WG.at[side, pl.ds(0, 5)], 0), (WG.at[side, pl.ds(5, 5)], 0), (F, ROWS * side))
             for side in range(2)], (0, 1, 2), 1, 5, 2)
        return carry

    lax.fori_loop(0, EARLY, wedge_cycle, 0)
    for side, tiles in ((0, (2, 3)), (1, (2, 3, 4))):
        for t in tiles:
            for q in range(3):
                for f in range(5):
                    F[f, q, tile(8 * t + ROWS * side), :] = WG[side, f, q, tile(8 * t), :]
                    if f < 2:
                        RL[f, q, tile(8 * t + ROWS * side), :] = WG[side, 5 + f, q, tile(8 * t), :]

    def merged(values):
        low = jnp.where(lane < 16, values[2], values[0])
        high = jnp.where(lane >= 108, pltpu.roll(values[2], 33, 1), values[1])
        return low, high

    def y_copy(e, d):
        rows = pl.ds(pl.multiple_of(OWN * e + 8 * lax.rem(y + d, 4), 8), 8)
        return pltpu.make_async_remote_copy(
            FB.at[:, :, rows], YR.at[e, 3 - d], ysend_sem.at[3 * e + d - 1],
            yrecv_sem.at[3 * e + 3 - d], device_id={"ens": y_peers[d - 1]},
            device_id_type=MESH_IDS)

    def z_copy(e):
        return pltpu.make_async_remote_copy(
            PART.at[e], ZR.at[ens], zsend_sem.at[e], zrecv_sem.at[ens],
            device_id={"ens": jnp.int32(e)}, device_id_type=MESH_IDS)

    def from_member(d):
        sender = lax.rem(ens + d, 8)
        return pltpu.make_async_remote_copy(
            PART.at[0], ZR.at[sender], zsend_sem.at[0], zrecv_sem.at[sender],
            device_id={"ens": sender}, device_id_type=MESH_IDS)

    def partial(blocks):
        for e in blocks:
            for d in (1, 2, 3):
                y_copy(e, d).wait_recv()
            own = pl.ds(pl.multiple_of(OWN * e + 8 * y, 8), 8)
            for f in range(3):
                for q in range(2):
                    v = [YR[e, n, f, q] for n in range(3)] + [FB[f, q, own, :]]
                    total = (v[0] + v[1]) + (v[2] + v[3])
                    mean = total * 0.25
                    x = [value - mean for value in v]
                    PART[e, 0, f, q] = total
                    PART[e, 1, f, q] = (x[0] * x[0] + x[1] * x[1]) + (x[2] * x[2] + x[3] * x[3])
            pl.when(ens != e)(z_copy(e).start)

    def chunk(pieces, split, earlier):
        regions = []
        for n, (e, count) in enumerate(pieces):
            base = BASE - 16 + OWN * e
            top = 8 * GROWS * n
            for t in range(4 * count + 4):
                for q in range(3):
                    for f in range(5):
                        G[f, q, tile(8 * t + top), :] = F[f, q, tile(8 * t + base), :]
                        G[5 + f, q, tile(8 * t + top), :] = RL[f, q, tile(8 * t + base), :]
            regions.append(((G.at[pl.ds(0, 5)], top), (G.at[pl.ds(5, 5)], top), (F, base)))
        last = 4 * pieces[0][1] + 3

        def cycle(n, carry):
            sweep_many(regions, (0, 1, 2), 1, last, CLAG)
            if earlier:
                pl.when(n == split)(lambda: partial(earlier))
            return carry

        lax.fori_loop(0, SUBCYCLES - EARLY, cycle, 0)

        for n, (e, count) in enumerate(pieces):
            for k in range(4 * count):
                o, r = OWN * e + 8 * k, 8 * GROWS * n + 8 * k + 16
                div = []
                for q in range(3):
                    a = G[5, q, tile(r + 1), :] - G[W, q, tile(r), :]
                    b = G[6, q, tile(r), :] - G[Z, q, tile(r + 1), :]
                    div.append(a + b)
                div = merged(div)
                w, z, p, m, t = (
                    merged([G[f, q, tile(r), :] for q in range(3)]) for f in (W, Z, PP, MM, TT))
                for q in range(2):
                    conc = IN[6, q, tile(o), :]
                    FB[0, q, tile(o), :] = jnp.clip(conc - conc * div[q], 0.0, 1.0)
                    FB[1, q, tile(o), :] = w[q] + z[q]
                    FB[2, q, tile(o), :] = w[q] - z[q]
                    OUT[0, q, tile(o), :] = (p[q] + m[q]) * (0.5 / BETA)
                    OUT[1, q, tile(o), :] = t[q] * (1.0 / BETA)
                    OUT[2, q, tile(o), :] = (p[q] - m[q]) * (0.25 / BETA)
            for block in range(e, e + count):
                for d in (1, 2, 3):
                    y_copy(block, d).start()

    chunk([(0, 2)], 0, ())
    chunk([(6, 2)], 0, ())
    chunk([(2, 1), (5, 1)], 3, (0, 1))
    chunk([(3, 2)], 4, (6, 7))
    partial((2, 5))
    partial((3, 4))

    for f in range(3):
        for q in range(2):
            for n in range(2):
                ZR[ens, n, f, q] = PART[ens, n, f, q]
    for d in range(1, 8):
        from_member(d).wait_recv()
    for k in range(4):
        rows = tile(8 * k)
        for f in range(3):
            for q in range(2):
                sa, sb = ZR[k, 0, f, q], ZR[4 + k, 0, f, q]
                ma, mb = ZR[k, 1, f, q], ZR[4 + k, 1, f, q]
                STAT[0, f, q, rows, :] = (sa + sb) * 0.125
                STAT[1, f, q, rows, :] = ((ma + mb) + (sa - sb) * (sa - sb) * 0.125) * 0.125
    for e in range(8):
        for d in (1, 2, 3):
            y_copy(e, d).wait_send()
        pl.when(ens != e)(z_copy(e).wait_send)


def emit(FB, OUT, STAT, vel_o, st_o, mean_o, var_o, sem):
    copies = []
    for q in range(2):
        columns = pl.ds(LANES * q, LANES)
        pairs = [(OUT.at[n, q], st_o.at[0, n]) for n in range(3)]
        pairs += [(FB.at[1 + n, q], vel_o.at[0, n]) for n in range(2)]
        for source, target in pairs:
            copies.append((source, target.at[:, columns]))
        for n, target in enumerate((mean_o, var_o)):
            copies.append((STAT.at[n, :, q], target.at[:, :, columns]))
    copies = [pltpu.make_async_copy(a, b, sem.at[n]) for n, (a, b) in enumerate(copies)]
    for copy in copies:
        copy.start()
    for copy in copies:
        copy.wait()


def body(velocity, stress, thickness, concentration, node_mass, wind_stress, ocean_current,
         ocean_mask, ice_blocks):
    f32 = jnp.float32
    hbm = pl.BlockSpec(memory_space=pltpu.HBM)
    vmem = pl.BlockSpec(memory_space=pltpu.VMEM)
    stat = jax.ShapeDtypeStruct((3, OWN, 2 * LANES), f32)
    big = [pltpu.with_memory_space_constraint(x, pltpu.HBM) for x in (velocity, stress, thickness, concentration, node_mass, wind_stress, ocean_current, ocean_mask, ice_blocks)]
    results = pl.pallas_call(
        kernel,
        out_shape=(
            jax.ShapeDtypeStruct((3, 2, ROWS, LANES), f32),
            jax.ShapeDtypeStruct((3, 2, ROWS, LANES), f32),
            jax.ShapeDtypeStruct((2, 3, 2, OWN, LANES), f32),
        ),
        in_specs=[hbm] * 9,
        out_specs=(vmem,) * 3,
        scratch_shapes=[
            pltpu.VMEM((14, 3, ALLOC, LANES), f32),
            pltpu.VMEM((5, 3, ALLOC, LANES), f32),
            pltpu.VMEM((2, 10, 3, 56, LANES), f32),
            pltpu.VMEM((12, 2, ROWS + 8, LANES), f32),
            pltpu.VMEM((2, ROWS, LANES), jnp.int32),
            pltpu.VMEM((2, 2, ROWS, LANES), f32),
            pltpu.VMEM((2, 2, ROWS, LANES), f32),
            pltpu.VMEM((10, 3, 16 * GROWS + 8, LANES), f32),
            pltpu.VMEM((8, 3, 3, 2, 8, LANES), f32),
            pltpu.VMEM((8, 2, 3, 2, 8, LANES), f32),
            pltpu.VMEM((8, 2, 3, 2, 8, LANES), f32),
            pltpu.SMEM((1, 8, 8), jnp.int32),
            pltpu.SemaphoreType.DMA((52,)),
            pltpu.SemaphoreType.DMA,
            pltpu.SemaphoreType.DMA((12,)),
            pltpu.SemaphoreType.DMA((12,)),
            pltpu.SemaphoreType.DMA((24,)),
            pltpu.SemaphoreType.DMA((24,)),
            pltpu.SemaphoreType.DMA((8,)),
            pltpu.SemaphoreType.DMA((8,)),
        ],
        compiler_params=pltpu.CompilerParams(
            collective_id=0, has_side_effects=True, vmem_limit_bytes=40 * 1024 * 1024),
        name="ice",
    )(*big)
    return pl.pallas_call(
        emit,
        out_shape=(
            jax.ShapeDtypeStruct(velocity.shape, f32),
            jax.ShapeDtypeStruct(stress.shape, f32),
            stat,
            stat,
        ),
        in_specs=[vmem] * 3,
        out_specs=(hbm,) * 4,
        scratch_shapes=[pltpu.SemaphoreType.DMA((14,))],
        compiler_params=pltpu.CompilerParams(vmem_limit_bytes=8 * 1024 * 1024),
        name="emit",
    )(*results)


def solution(mesh):
    member, field = P("ens", None, "gy", "gx"), P("ens", "gy", "gx")
    placed = (member, member, field, field, field, member, member, P("gy", "gx"), field)
    block = P(None, ("gy", "ens"), "gx")
    return jax.shard_map(
        body, mesh=mesh, in_specs=placed, out_specs=(member, member, block, block),
        check_vma=False)
```
